32 devices in a mesh: curve: 4 (over y, core), group: 8 (over z, x).
Axes of the slice: x: 2, y: 2, z: 4, core: 2. Of those that a mesh axis runs over, the one named last changes fastest.
Arguments:
- right_side: float32 [125, 16384], P(None, ('curve', 'group')), may hold values from -6 to 6, as said below
- conductivity: float32 [16384], P(('curve', 'group')), may hold values from 0.3 to 3
- destination: int32 [16384], P(('curve', 'group')), may hold values from 0 to 16383, as said below
- neighbour: int32 [6, 16384], P(None, ('curve', 'group')), may hold values from -1 to 1023, as said below
- orientation: int32 [6, 16384], P(None, ('curve', 'group')), may hold values from 0 to 3, as said below
- send_list: int32 [2, 8192], P(None, ('curve', 'group')), may hold values from 0 to 511, as said below
Outputs:
- solution: float32 [125, 16384], P(None, ('curve', 'group'))
- residual: float32 [125, 16384], P(None, ('curve', 'group'))
The draws below stay inside these ranges and needn't reach their ends.
Inputs may be any that keep to these rules, and one draw needn't show every extreme that they name: `right_side`: custom normal-like values. `destination`: A permutation of all cells. Devices are ordered along the curve with curve slowest; every cell's new device is its old device or the one just before or after it. From each device at most 64 cells go to the next device and exactly as many come back from it; 64 is reached at some pair of neighbouring devices in every draw. `neighbour`: values below 512 are local cells of the same device. Only face 0 may name a slot from 512 to 512 + 256 - 1 (filled by the previous device from its send_list row 1), only face 1 a slot from 768 up (filled by the next device from its send_list row 0). Faces are paired: the cell across face f sees this cell across face f xor 1. -1 only at the domain boundary; the first device has no partner across its face 0 slots and the last none across face 1 slots. `orientation`: both sides of a shared face carry the same code; ignored where neighbour is -1. `send_list`: per device 256 distinct local cells in each row.
All inputs are finite; a program needn't handle non-finite values.
Results may differ from the reference program's by a relative error of at most 0.00015.
Values sent between devices are 32-bit elements; how exact they have to be, the bound alone decides.
A program may use at most 64 MiB of HBM per device.

```python
import math
import jax
import jax.numpy as jnp
from jax import lax

CELLS_DEV = 512
SIDE = 16
NODES = 5
ITERS = 2
BLOCK = 125
GHOST = 256
MOVE = 64
RANKS = 32
CELLS = 16384


def draw_right_side(key, part):
    key_rough = jax.random.fold_in(jax.random.fold_in(key, 3), 0)
    rough = jax.random.normal(key_rough, (BLOCK, CELLS), jnp.float32)
    return jnp.clip(rough, -6.0, 6.0)


def draw_destination(key, part):
    base_key = jax.random.fold_in(key, 29)
    key_swap, key_pick, key_rank, key_order = jax.random.split(base_key, 4)
    swap_counts = jax.random.randint(key_swap, (RANKS - 1,), 0, MOVE + 1).astype(jnp.int32)
    forced_at = jax.random.randint(key_pick, (), 0, RANKS - 1)
    swap_counts = swap_counts.at[forced_at].set(MOVE)
    zero_pad = jnp.zeros((1,), jnp.int32)
    to_left = jnp.concatenate([zero_pad, swap_counts])[:, None]
    to_right = jnp.concatenate([swap_counts, zero_pad])[:, None]
    local_rank = jax.vmap(lambda one_key: jax.random.permutation(one_key, CELLS_DEV))(jax.random.split(key_rank, RANKS)).astype(jnp.int32)
    old_owner = jnp.arange(RANKS, dtype=jnp.int32)[:, None]
    target = jnp.where(local_rank < to_left, old_owner - 1, jnp.where(local_rank >= CELLS_DEV - to_right, old_owner + 1, old_owner)).reshape(CELLS)
    shuffled = jax.random.permutation(key_order, CELLS).astype(jnp.int32)
    new_order = shuffled[jnp.argsort(target[shuffled], stable=True)]
    return jnp.zeros((CELLS,), jnp.int32).at[new_order].set(jnp.arange(CELLS, dtype=jnp.int32))


def mesh_arrays(key):
    base_key = jax.random.fold_in(key, 17)
    key_perm, key_code = jax.random.split(base_key)
    ghost_count = SIDE * SIDE
    layers = CELLS_DEV // ghost_count
    site_cell = jax.vmap(lambda one_key: jax.random.permutation(one_key, CELLS_DEV))(jax.random.split(key_perm, RANKS)).astype(jnp.int32)
    face_codes = jax.random.randint(key_code, (RANKS, CELLS_DEV, 3), 0, 4).astype(jnp.int32)
    site_ids = jnp.arange(CELLS_DEV, dtype=jnp.int32)
    layer_pos = (site_ids // ghost_count)[None, :]
    row_pos = (site_ids // SIDE % SIDE)[None, :]
    col_pos = (site_ids % SIDE)[None, :]
    plane_slot = row_pos * SIDE + col_pos
    rank_ids = jnp.arange(RANKS, dtype=jnp.int32)[:, None]

    def ahead_by(table, step):
        return jnp.roll(table, -step, axis=1)

    def behind_by(table, step):
        return jnp.roll(table, step, axis=1)
    face_zero = jnp.where(layer_pos > 0, behind_by(site_cell, ghost_count), jnp.where(rank_ids > 0, CELLS_DEV + plane_slot, -1))
    face_one = jnp.where(layer_pos < layers - 1, ahead_by(site_cell, ghost_count), jnp.where(rank_ids < RANKS - 1, CELLS_DEV + ghost_count + plane_slot, -1))
    face_two = jnp.where(row_pos > 0, behind_by(site_cell, SIDE), -1)
    face_three = jnp.where(row_pos < SIDE - 1, ahead_by(site_cell, SIDE), -1)
    face_four = jnp.where(col_pos > 0, behind_by(site_cell, 1), -1)
    face_five = jnp.where(col_pos < SIDE - 1, ahead_by(site_cell, 1), -1)
    code_x = face_codes[..., 0]
    code_y = face_codes[..., 1]
    code_z = face_codes[..., 2]
    previous_x = jnp.roll(jnp.roll(code_x, 1, axis=0), -(layers - 1) * ghost_count, axis=1)
    code_zero = jnp.where(layer_pos > 0, behind_by(code_x, ghost_count), previous_x)
    code_two = jnp.where(row_pos > 0, behind_by(code_y, SIDE), code_y)
    code_four = jnp.where(col_pos > 0, behind_by(code_z, 1), code_z)
    inverse = jnp.argsort(site_cell, axis=1, stable=True)
    neighbour_sites = jnp.stack([face_zero, face_one, face_two, face_three, face_four, face_five]).astype(jnp.int32)
    code_sites = jnp.stack([code_zero, code_x, code_two, code_y, code_four, code_z]).astype(jnp.int32)
    neighbour = jnp.take_along_axis(neighbour_sites, inverse[None], axis=2).reshape(6, CELLS)
    orientation = jnp.take_along_axis(code_sites, inverse[None], axis=2).reshape(6, CELLS)
    send_list = jnp.stack([site_cell[:, :ghost_count], site_cell[:, (layers - 1) * ghost_count:]]).reshape(2, RANKS * ghost_count)
    return (neighbour, orientation, send_list)


def draw_neighbour(key, part):
    return mesh_arrays(key)[0]


def draw_orientation(key, part):
    return mesh_arrays(key)[1]


def draw_send_list(key, part):
    return mesh_arrays(key)[2]


def levels(stream_key, dims, cuts, smallest, high):
    def one(dim, shards_of):
        heights = jax.random.uniform(jax.random.fold_in(jax.random.fold_in(stream_key, 6), dim), (shards_of,), jnp.float32, smallest / len(cuts), high / len(cuts))
        return jnp.repeat(jnp.exp(heights), dims[dim] // shards_of).reshape((-1,) + (1,) * (len(dims) - dim - 1))

    gain = one(*cuts[0])
    for cut in cuts[1:]:
        gain = gain * one(*cut)
    return gain


def setup_inputs(seed: int = 0) -> dict:
    arg_keys = jax.random.split(jax.random.key(seed), 7)
    right_side = draw_right_side(jax.random.fold_in(arg_keys[6], 71), 0)
    conductivity = jnp.clip(jnp.exp(math.log(3.0) - 2.3025851 * jax.random.uniform(arg_keys[1], (CELLS,), jnp.float32) ** levels(arg_keys[1], (CELLS,), ((0, 32),), -0.2, 0.2)), 0.3, 3.0)
    destination = draw_destination(jax.random.fold_in(arg_keys[6], 71), 0)
    neighbour = draw_neighbour(jax.random.fold_in(arg_keys[6], 71), 0)
    orientation = draw_orientation(jax.random.fold_in(arg_keys[6], 71), 0)
    send_list = draw_send_list(jax.random.fold_in(arg_keys[6], 71), 0)
    return {"right_side": right_side, "conductivity": conductivity, "destination": destination, "neighbour": neighbour, "orientation": orientation, "send_list": send_list}


PENALTY = 80.0
HIGHEST = lax.Precision.HIGHEST
GAUSS_POINTS = (-0.9061798459386640, -0.5384693101056831, 0.0, 0.5384693101056831, 0.9061798459386640)
GAUSS_WEIGHTS = (0.2369268850561891, 0.4786286704993665, 0.5688888888888889, 0.4786286704993665, 0.2369268850561891)


def lagrange_value(points, position, location):
    product_value = 1.0
    for other_id in range(len(points)):
        if other_id != position:
            product_value = product_value * (location - points[other_id]) / (points[position] - points[other_id])
    return product_value


def lagrange_slope(points, position, location):
    slope_sum = 0.0
    for skipped in range(len(points)):
        if skipped == position:
            continue
        addend = 1.0 / (points[position] - points[skipped])
        for other_id in range(len(points)):
            if other_id != position and other_id != skipped:
                addend = addend * (location - points[other_id]) / (points[position] - points[other_id])
        slope_sum = slope_sum + addend
    return slope_sum


def basis_tables():
    points = [0.5 * (value + 1.0) for value in GAUSS_POINTS]
    weights = [0.5 * value for value in GAUSS_WEIGHTS]
    count = len(points)
    slopes = [[lagrange_slope(points, column, points[row_id]) for column in range(count)] for row_id in range(count)]
    start_value = [lagrange_value(points, column, 0.0) for column in range(count)]
    end_value = [lagrange_value(points, column, 1.0) for column in range(count)]
    start_slope = [-lagrange_slope(points, column, 0.0) for column in range(count)]
    end_slope = [lagrange_slope(points, column, 1.0) for column in range(count)]
    listed = (weights, slopes, start_value, end_value, start_slope, end_slope)
    return tuple(jnp.asarray(table, jnp.float32) for table in listed)


def face_vectors(face_id, tables):
    if face_id % 2:
        return tables[3], tables[5]
    return tables[2], tables[4]


def face_data(block_field, conduct, face_id, tables):
    trace_vec, normal_vec = face_vectors(face_id, tables)
    axis_id = face_id // 2
    trace_value = jnp.tensordot(trace_vec, block_field, axes=([0], [axis_id]), precision=HIGHEST)
    trace_flux = conduct * jnp.tensordot(normal_vec, block_field, axes=([0], [axis_id]), precision=HIGHEST)
    return trace_value, trace_flux


def spread_back(vector, face_part, axis_id):
    bcast_shape = [1, 1, 1, 1]
    bcast_shape[axis_id] = NODES
    return vector.reshape(bcast_shape) * jnp.expand_dims(face_part, axis_id)


def volume_term(block_field, conduct, tables):
    weights, slopes = tables[0], tables[1]
    weight_3d = (weights[:, None, None] * weights[None, :, None] * weights[None, None, :])[..., None]
    result = weight_3d * block_field
    forward = ("qp,pjkc->qjkc", "qp,ipkc->iqkc", "qp,ijpc->ijqc")
    backward = ("qp,qjkc->pjkc", "qp,iqkc->ipkc", "qp,ijqc->ijpc")
    for axis_id in range(3):
        grads = jnp.einsum(forward[axis_id], slopes, block_field, precision=HIGHEST)
        result = result + jnp.einsum(backward[axis_id], slopes, weight_3d * conduct * grads, precision=HIGHEST)
    return result


def face_term(trace_value, trace_flux, conduct, other_value, other_flux, other_conduct, partner, orient_code, face_id, tables):
    weights = tables[0]
    trace_vec, normal_vec = face_vectors(face_id, tables)
    axis_id = face_id // 2
    flip_first = (orient_code % 2) == 1
    flip_second = (orient_code // 2) == 1
    other_value = jnp.where(flip_first, other_value[::-1], other_value)
    other_value = jnp.where(flip_second, other_value[:, ::-1], other_value)
    other_flux = jnp.where(flip_first, other_flux[::-1], other_flux)
    other_flux = jnp.where(flip_second, other_flux[:, ::-1], other_flux)
    outside = partner < 0
    other_value = jnp.where(outside, -trace_value, other_value)
    other_flux = jnp.where(outside, -trace_flux, other_flux)
    other_conduct = jnp.where(outside, conduct, other_conduct)
    penalty = PENALTY * jnp.maximum(conduct, other_conduct)
    trace_jump = trace_value - other_value
    mean_flux = 0.5 * (trace_flux - other_flux)
    face_weight = (weights[:, None] * weights[None, :])[:, :, None]
    first_part = spread_back(trace_vec, face_weight * (penalty * trace_jump - mean_flux), axis_id)
    return first_part + spread_back(normal_vec, face_weight * (-0.5 * conduct * trace_jump), axis_id)


def global_partners(neighbour, send_list):
    cell_ids = jnp.arange(CELLS, dtype=jnp.int32)
    owner = cell_ids // CELLS_DEV
    lower = jnp.maximum(owner - 1, 0)
    upper = jnp.minimum(owner + 1, RANKS - 1)
    left_slot = jnp.clip(neighbour - CELLS_DEV, 0, GHOST - 1)
    right_slot = jnp.clip(neighbour - CELLS_DEV - GHOST, 0, GHOST - 1)
    from_left = lower * CELLS_DEV + send_list[1][lower * GHOST + left_slot]
    from_right = upper * CELLS_DEV + send_list[0][upper * GHOST + right_slot]
    local_ids = owner * CELLS_DEV + neighbour
    joined = jnp.where(neighbour < CELLS_DEV, local_ids, jnp.where(neighbour < CELLS_DEV + GHOST, from_left, from_right))
    return jnp.where(neighbour < 0, -1, joined).astype(jnp.int32)


def operate(block_field, conduct, partners, orientation, tables):
    faces = [face_data(block_field, conduct, face_id, tables) for face_id in range(6)]
    result = volume_term(block_field, conduct, tables)
    for face_id in range(6):
        partner = partners[face_id]
        safe_idx = jnp.where(partner < 0, 0, partner)
        other_value, other_flux = faces[face_id ^ 1]
        result = result + face_term(faces[face_id][0], faces[face_id][1], conduct,
                                    other_value[:, :, safe_idx], other_flux[:, :, safe_idx], conduct[safe_idx],
                                    partner, orientation[face_id], face_id, tables)
    return result


def reference(right_side, conductivity, destination, neighbour, orientation, send_list):
    tables = basis_tables()
    placed = jnp.zeros((BLOCK, CELLS), jnp.float32).at[:, destination].set(right_side)
    conduct = jnp.zeros((CELLS,), jnp.float32).at[destination].set(conductivity)
    partners = global_partners(neighbour, send_list)
    source = placed.reshape(NODES, NODES, NODES, CELLS)
    solution = jnp.zeros_like(source)
    residual = source
    direction = source
    norm_now = jnp.sum(residual * residual)
    for step in range(ITERS):
        image = operate(direction, conduct, partners, orientation, tables)
        step_size = norm_now / jnp.sum(direction * image)
        solution = solution + step_size * direction
        residual = residual - step_size * image
        if step + 1 < ITERS:
            norm_next = jnp.sum(residual * residual)
            direction = residual + (norm_next / norm_now) * direction
            norm_now = norm_next
    return solution.reshape(BLOCK, CELLS), residual.reshape(BLOCK, CELLS)
```

```python
import functools

import jax
import jax.numpy as jnp
import numpy as np
from jax import lax
from jax.experimental import pallas as pl
from jax.experimental.pallas import tpu as pltpu
from jax.sharding import PartitionSpec as P

NODES = 5
BLOCK = 125
MOVE = 64
UNROLLED = 64
VMEM_LIMIT = 24 * 1024 * 1024
PENALTY = 80.0
MESH = pl.DeviceIdType.MESH
BF = jnp.bfloat16
F32 = jnp.float32

ROWS = 128
KAPPA = 125
TAG = 126
PART = 32
FACE = 2 * PART
FACE_KAPPA = 25
FACE_TAG = 26
HALO = PART + 24
FACE_LAST = 27

GAUSS_POINTS = (-0.906179845938664, -0.5384693101056831, 0.0, 0.5384693101056831, 0.906179845938664)
GAUSS_WEIGHTS = (
    0.2369268850561891,
    0.4786286704993665,
    0.5688888888888889,
    0.4786286704993665,
    0.2369268850561891,
)


def lagrange_value(points, position, location):
    out = 1.0
    for other in range(len(points)):
        if other != position:
            out = out * (location - points[other]) / (points[position] - points[other])
    return out


def lagrange_slope(points, position, location):
    total = 0.0
    for skipped in range(len(points)):
        if skipped == position:
            continue
        addend = 1.0 / (points[position] - points[skipped])
        for other in range(len(points)):
            if other != position and other != skipped:
                addend = addend * (location - points[other]) / (points[position] - points[other])
        total = total + addend
    return total


def along_axis(matrix, axis):
    five = np.eye(NODES)
    plane = np.eye(NODES * NODES)
    if axis == 0:
        return np.kron(matrix, plane)
    if axis == 1:
        return np.kron(five, np.kron(matrix, five))
    return np.kron(plane, matrix)


def split_table(table):
    high = table.astype(BF)
    low = (table - high.astype(np.float64)).astype(BF)
    return high, low


def tables():
    points = [0.5 * (value + 1.0) for value in GAUSS_POINTS]
    weights = np.array([0.5 * value for value in GAUSS_WEIGHTS])
    slopes = np.array([[lagrange_slope(points, p, points[q]) for p in range(NODES)] for q in range(NODES)])
    ends = [np.array([lagrange_value(points, p, at) for p in range(NODES)]) for at in (0.0, 1.0)]
    normals = [
        np.array([sign * lagrange_slope(points, p, at) for p in range(NODES)])
        for sign, at in ((-1.0, 0.0), (1.0, 1.0))
    ]
    cell_weight = np.kron(weights, np.kron(weights, weights))
    stiffness = np.zeros((BLOCK, BLOCK))
    for axis in range(3):
        grad = along_axis(slopes, axis)
        stiffness += grad.T @ (cell_weight[:, None] * grad)
    half = np.sqrt(0.5)
    parity_rows = np.zeros((NODES, NODES))
    for row, (a, b, sign) in enumerate(((0, 4, 1), (1, 3, 1), (2, 2, 1), (0, 4, -1), (1, 3, -1))):
        if a == b:
            parity_rows[row, a] = 1.0
        else:
            parity_rows[row, a] = half
            parity_rows[row, b] = sign * half
    parity = np.array([0, 0, 0, 1, 1])
    row_weight = weights[[0, 1, 2, 0, 1]]
    both = np.kron(parity_rows, parity_rows)
    count = NODES * NODES
    trace = np.zeros((6 * FACE, ROWS))
    for face in range(6):
        start = face * FACE
        trace[start : start + count, :BLOCK] = both @ along_axis(ends[face % 2][None, :], face // 2)
        trace[start + PART : start + PART + count, :BLOCK] = both @ along_axis(
            normals[face % 2][None, :], face // 2
        )
    lift = trace.T.copy()
    for face in range(6):
        trace[face * FACE + FACE_KAPPA, KAPPA] = 1.0
    first = np.zeros((6 * FACE + ROWS, ROWS))
    first[: 6 * FACE] = trace
    first[6 * FACE : 6 * FACE + BLOCK, :BLOCK] = stiffness
    high, low = split_table(first)
    forward = np.concatenate([high, high, low], 1)
    high, low = split_table(lift)
    backward = np.concatenate([high, low], 0)
    columns = np.zeros((ROWS, ROWS), np.float32)
    columns[:BLOCK, 0] = cell_weight
    columns[:count, 1] = np.kron(row_weight, row_weight)
    columns[:count, 2] = 2.0 * np.kron(parity, np.ones(NODES))
    columns[:count, 3] = 2.0 * np.kron(np.ones(NODES), parity)
    return forward, backward, columns


def split_two(value):
    high = value.astype(BF)
    low = (value - high.astype(F32)).astype(BF)
    return high, low


def split_three(value):
    high = value.astype(BF)
    rest = value - high.astype(F32)
    mid = rest.astype(BF)
    return high, mid, (rest - mid.astype(F32)).astype(BF)


def one_hot(left, right):
    return jnp.where(left == right, 1.0, 0.0).astype(BF)


def dot(left, right):
    return jnp.dot(left, right, preferred_element_type=F32)


def dot_last(left, right):
    return lax.dot_general(left, right, (((1,), (1,)), ((), ())), preferred_element_type=F32)


def iota(shape, dim):
    return lax.broadcasted_iota(jnp.int32, shape, dim)


def kernel(
    shape,
    rhs_hbm,
    cond_hbm,
    dest_hbm,
    neigh_hbm,
    orient_hbm,
    list_hbm,
    forward_hbm,
    backward_hbm,
    column_hbm,
    basis,
    linear_ref,
    square_ref,
    rhs_ref,
    cond_ref,
    dest_ref,
    neigh_ref,
    orient_ref,
    list_ref,
    forward_ref,
    backward_ref,
    column_ref,
    payload,
    local_hot,
    ghost_hot,
    send_hot,
    packed,
    moved,
    far_out,
    far_in,
    halo_out,
    halo_in,
    sums,
    kept,
    load_sem,
    move_send,
    move_recv,
    far_send,
    far_recv,
    halo_send,
    halo_recv,
    sum_send,
    sum_recv,
):
    curve, group = shape
    ranks = curve * group
    cells = rhs_ref.shape[1]
    ghost = list_ref.shape[1]
    me = lax.axis_index("curve") * group + lax.axis_index("group")

    def place(rank):
        return (rank // group, lax.rem(rank, group))

    def other(step):
        return place(lax.rem(me + step, ranks))

    class Exchange:
        def __init__(self, source, target, send_sem, recv_sem, reach):
            self.there = (me >= reach, me + reach < ranks)
            self.copies = [
                pltpu.make_async_remote_copy(
                    src_ref=source.at[side],
                    dst_ref=target.at[1 - side],
                    send_sem=send_sem.at[side],
                    recv_sem=recv_sem.at[1 - side],
                    device_id=device,
                    device_id_type=MESH,
                )
                for side, device in ((0, other(ranks - reach)), (1, other(reach)))
            ]

        def start(self):
            for side in range(2):
                pl.when(self.there[side])(self.copies[side].start)

        def arrive(self, side):
            pl.when(self.there[side])(self.copies[1 - side].wait_recv)

        def leave(self):
            for side in range(2):
                pl.when(self.there[side])(self.copies[side].wait_send)

    def clear(reach, refs):
        for side, missing in ((0, me < reach), (1, me + reach >= ranks)):

            @pl.when(missing)
            def _():
                for ref in refs:
                    ref[side] = jnp.zeros(ref.shape[1:], ref.dtype)

    barrier = pltpu.get_barrier_semaphore()

    my_curve, my_group = lax.axis_index("curve"), lax.axis_index("group")

    def for_each_other(act):
        def one(to_group):
            for step in range(curve):
                to = (lax.rem(my_curve + step, curve), to_group)
                if step:
                    act(to)
                else:
                    pl.when(to_group != my_group)(functools.partial(act, to))

        if ranks <= UNROLLED:
            for to_group in range(group):
                one(to_group)
        else:
            pl.loop(0, group)(one)

    for_each_other(
        lambda device: pl.semaphore_signal(barrier, inc=1, device_id=device, device_id_type=MESH)
    )

    loads = [
        pltpu.make_async_copy(source, target, load_sem.at[index])
        for index, (source, target) in enumerate(
            (
                (dest_hbm, dest_ref),
                (list_hbm, list_ref),
                (cond_hbm, cond_ref),
                (rhs_hbm, rhs_ref),
                (forward_hbm, forward_ref),
                (neigh_hbm, neigh_ref),
                (orient_hbm, orient_ref),
                (column_hbm, column_ref),
                (backward_hbm, backward_ref),
            )
        )
    ]
    for load in loads:
        load.start()
    clear(1, (moved, halo_in.at[0], halo_in.at[1]))
    clear(2, (far_in,))
    for load in loads[:4]:
        load.wait()

    def faces_of(stacked, kappa, first, last):
        part = dot(forward_ref[first * FACE : last * FACE, :], stacked)
        own, halves = [], []
        for index in range(last - first):
            value = part[index * FACE : index * FACE + PART]
            flux = kappa * part[index * FACE + PART : (index + 1) * FACE]
            own.append((value, flux))
            halves.append(jnp.concatenate(split_two(jnp.concatenate([value, flux], 0)), 0))
        return own, halves

    offset = dest_ref[...] - me * cells
    goes_left = offset < 0
    goes_right = offset >= cells
    slot = jnp.where(goes_left, offset + cells, jnp.where(goes_right, offset - cells, offset))
    payload[0:BLOCK, :] = rhs_ref[...]
    payload[KAPPA : KAPPA + 1, :] = cond_ref[...]
    payload[TAG : TAG + 1, :] = (slot + 1).astype(F32)
    payload[TAG + 1 : TAG + 2, :] = jnp.zeros((1, cells), F32)
    high, mid, low = split_three(payload[...])
    parts = jnp.concatenate([high, mid, low], 0)
    row8 = iota((8, cells), 0)
    leaving = jnp.where(
        row8 == 0,
        jnp.where(goes_left, 1.0, 0.0),
        jnp.where(row8 == 1, jnp.where(goes_right, 1.0, 0.0), 0.0),
    ).astype(BF)
    triangle = jnp.where(iota((cells, cells), 0) <= iota((cells, cells), 1), 1.0, 0.0).astype(BF)
    order = dot(leaving, triangle).astype(jnp.int32) - 1
    slots = iota((MOVE, cells), 0)
    pick = jnp.concatenate(
        [
            one_hot(jnp.where(goes_left, order[0:1], -1), slots),
            one_hot(jnp.where(goes_right, order[1:2], -1), slots),
        ],
        0,
    )
    chosen = dot_last(pick, parts)
    chosen = chosen[:, :ROWS] + chosen[:, ROWS : 2 * ROWS] + chosen[:, 2 * ROWS :]
    packed[0] = chosen[:MOVE]
    packed[1] = chosen[MOVE:]

    pl.semaphore_wait(barrier, ranks - 1)

    moves = Exchange(packed, moved, move_send, move_recv, 1)
    moves.start()

    for load in loads[4:]:
        load.wait()

    old_halves = faces_of(jnp.concatenate([high, mid, high], 0), cond_ref[...], 0, 2)[1]
    offset_column = jnp.broadcast_to(offset.astype(F32), (8, cells)).T[:, 0:1]
    lists = list_ref[...].astype(F32)
    halo_rows = iota((HALO, ghost), 0)

    def shrink(out):
        out = out[:FACE] + out[FACE:]
        return jnp.where(halo_rows == FACE_LAST, out[HALO : HALO + 1], out[:HALO])

    def widen(message):
        last = message[FACE_LAST : FACE_LAST + 1]
        rest = jnp.where(iota((FACE - HALO, ghost), 0) == 0, last, 0.0)
        return jnp.concatenate([message, rest], 0)

    for side in range(2):
        hot = one_hot(offset_column, lists[side : side + 1, :])
        out = dot(old_halves[side], hot)
        halo_out[0, side] = jnp.where(
            halo_rows == FACE_TAG, lists[side : side + 1, :], shrink(out)
        )
    lanes = iota((2 * MOVE, ROWS), 1)
    tagged = jnp.where(lanes == FACE_TAG, chosen[:, TAG : TAG + 1], 0.0)
    leaving_low = dot_last(pick, old_halves[0]) + tagged
    leaving_high = dot_last(pick, old_halves[1]) + tagged
    leaving_low = leaving_low[:, :FACE] + leaving_low[:, FACE:]
    leaving_high = leaving_high[:, :FACE] + leaving_high[:, FACE:]
    middle = MOVE // 2
    far_out[0] = jnp.concatenate([leaving_low[:middle], leaving_low[middle:MOVE]], 1)
    far_out[1] = jnp.concatenate([leaving_high[MOVE : MOVE + middle], leaving_high[MOVE + middle :]], 1)

    halos = Exchange(halo_out.at[0], halo_in.at[0], halo_send.at[0], halo_recv.at[0], 1)
    fars = Exchange(far_out, far_in, far_send, far_recv, 2)
    fars.start()
    halos.start()

    stay = one_hot(iota((cells, cells), 0), offset)
    arrived = dot_last(parts, stay)
    cell_rows = iota((cells, cells), 0)
    ghost_rows = iota((ghost, cells), 0)
    for face in range(6):
        local_hot[face] = one_hot(neigh_ref[face : face + 1, :], cell_rows)
    for side in range(2):
        ghost_hot[side] = one_hot(
            neigh_ref[side : side + 1, :] - (cells + side * ghost), ghost_rows
        )
        send_hot[side] = one_hot(list_ref[side : side + 1, :], iota((cells, ghost), 0))

    for side in range(2):
        moves.arrive(side)
    record = moved[...].reshape(2 * MOVE, ROWS)
    landing = record[:, TAG : TAG + 1].astype(jnp.int32) - 1
    record_parts = jnp.concatenate(split_three(record.T), 0)
    arrived = arrived + dot(record_parts, one_hot(landing, iota((2 * MOVE, cells), 1)))
    arrived = arrived[:ROWS] + arrived[ROWS : 2 * ROWS] + arrived[2 * ROWS :]
    rows = iota((ROWS, cells), 0)
    field = jnp.where(rows < BLOCK, arrived, 0.0)
    kappa = arrived[KAPPA : KAPPA + 1]
    cell_weight = column_ref[:, 0:1]
    face_weight = column_ref[0:PART, 1:2]
    first_odd = column_ref[0:PART, 2:3]
    second_odd = column_ref[0:PART, 3:4]

    def signs(face):
        code = orient_ref[face : face + 1, :]
        first_bit = jnp.where(lax.rem(code, 2) == 1, 1.0, 0.0)
        second_bit = jnp.where(code >= 2, 1.0, 0.0)
        return (1.0 - first_odd * first_bit) * (1.0 - second_odd * second_bit)

    def outer(face):
        return jnp.where(neigh_ref[face : face + 1, :] < 0, 1.0, 0.0)

    def coefficients(face, own, near):
        value, flux = own
        sign = signs(face)
        outside = outer(face)
        near = near[:FACE] + near[FACE:]
        near_kappa = near[FACE_KAPPA : FACE_KAPPA + 1] + outside * kappa
        penalty = PENALTY * jnp.maximum(kappa, near_kappa)
        jump = value - (sign * near[:PART] - outside * value)
        mean = flux - (sign * near[PART:] - outside * flux)
        scaled = -0.5 * (face_weight * jump)
        first = face_weight * (penalty * jump - 0.5 * mean)
        return (first, kappa * scaled), (jump, mean, first, scaled)

    def lifted(terms, first, last):
        high, low = split_two(jnp.concatenate(terms, 0))
        both = dot(backward_ref[:, first * FACE : last * FACE], high)
        rest = dot(backward_ref[0:ROWS, first * FACE : last * FACE], low)
        return both[:ROWS] + both[ROWS:] + rest

    def stack(field):
        high, low = split_two(jnp.where(rows == KAPPA, kappa, field))
        return jnp.concatenate([high, low, high], 0)

    def inner(field, stacked, halves):
        more_own, more_halves = faces_of(stacked, kappa, 2, 6)
        terms = []
        for face in range(2, 6):
            near = dot(more_halves[(face ^ 1) - 2], local_hot[face])
            terms += coefficients(face, more_own[face - 2], near)[0]
        result = lifted(terms, 2, 6)
        stiff = dot(forward_ref[6 * FACE :, :], stacked)
        result = result + cell_weight * field + kappa * stiff
        return result, [dot(halves[face ^ 1], local_hot[face]) for face in range(2)]

    def with_ghosts(near, ghosts, side):
        return near + dot(jnp.concatenate(split_two(ghosts), 0), ghost_hot[side])

    def down(value):
        return jnp.sum(value, 0, keepdims=True)

    def across(value):
        return jnp.sum(value, 1, keepdims=True)

    basis[0] = field
    stacked = stack(field)
    own, halves = faces_of(stacked, kappa, 0, 2)
    result, near = inner(field, stacked, halves)
    for side in range(2):
        halos.arrive(side)
        fars.arrive(side)
    terms = []
    for face in range(2):
        ghosts = widen(halo_in[0, face])
        gone = leaving_high[:MOVE] if face == 0 else leaving_low[MOVE:]
        far = far_in[face]
        wide = jnp.concatenate([far[:, :FACE], far[:, FACE:], gone], 0)
        hot = one_hot(wide[:, FACE_TAG : FACE_TAG + 1] - 1.0, ghosts[FACE_TAG : FACE_TAG + 1])
        placed = dot(jnp.concatenate(split_two(wide.T), 0), hot)
        ghosts = ghosts + placed[:FACE] + placed[FACE:]
        terms += coefficients(face, own[face], with_ghosts(near[face], ghosts, face))[0]
    image = result + lifted(terms, 0, 2)

    stacked = stack(image)
    own, halves = faces_of(stacked, kappa, 0, 2)
    for side in range(2):
        halo_out[1, side] = shrink(dot(halves[side], send_hot[side]))
    images = Exchange(halo_out.at[1], halo_in.at[1], halo_send.at[1], halo_recv.at[1], 1)
    images.start()
    basis[1] = image
    result, near = inner(image, stacked, halves)
    value, flux = own[1]
    edge = 2.0 * outer(1) * down(face_weight * (value * (PENALTY * kappa * value - flux)))
    found = [across(down(field * field)), across(down(field * image)), across(down(image * image))]
    outside = outer(0) > 0.0
    kept[...] = near[0]
    _, (jump, mean, first, scaled) = coefficients(0, own[0], near[0])

    inside = jnp.where(outside, own[0][0], jump) * first + jnp.where(outside, own[0][1], mean) * scaled
    inside = jnp.where(neigh_ref[0:1, :] < cells, down(inside), 0.0)
    found.append(across(down(image * result) + edge + inside))
    lane = iota((1, ROWS), 1)
    message = jnp.zeros((1, ROWS), F32)
    for index, value in enumerate(found):
        message = jnp.where(lane == index, value, message)
    across_edge = dot_last(halves[0], ghost_hot[0])
    across_edge = across_edge[:FACE] + across_edge[FACE:]
    code = orient_ref[0:1, :]
    bit_rows = iota((8, cells), 0)
    bits = jnp.where(
        bit_rows == 0, lax.rem(code, 2), jnp.where(bit_rows == 1, jnp.where(code >= 2, 1, 0), 1)
    )
    bits = dot_last(bits.astype(F32).astype(BF), ghost_hot[0])
    slot_sign = (1.0 - first_odd * bits[0:1]) * (1.0 - second_odd * bits[1:2])
    slot_weight = face_weight * bits[2:3]
    slot_kappa = across_edge[FACE_KAPPA : FACE_KAPPA + 1]

    images.arrive(0)
    ghosts = widen(halo_in[1, 0])
    penalty = PENALTY * jnp.maximum(slot_kappa, ghosts[FACE_KAPPA : FACE_KAPPA + 1])
    jump = across_edge[:PART] - slot_sign * ghosts[:PART]
    mean = across_edge[PART:] - slot_sign * ghosts[PART:]
    shared = across(down(slot_weight * (jump * (penalty * jump - mean))))
    sums[me] = message + jnp.where(lane == 3, shared, 0.0)

    for_each_other(
        lambda device: pltpu.make_async_remote_copy(
            src_ref=sums.at[me],
            dst_ref=sums.at[me],
            send_sem=sum_send,
            recv_sem=sum_recv,
            device_id=device,
            device_id_type=MESH,
        ).start()
    )

    images.arrive(1)
    terms = []
    near[0] = kept[...]
    for face in range(2):
        terms += coefficients(face, own[face], with_ghosts(near[face], widen(halo_in[1, face]), face))[0]
    basis[2] = result + lifted(terms, 0, 2)
    for copies in (moves, halos, fars, images):
        copies.leave()
    rest = sums.at[pl.ds(1, ranks - 1)]
    pltpu.make_async_copy(rest, rest, sum_send).wait()
    pltpu.make_async_copy(rest, rest, sum_recv).wait()
    summed = jnp.sum(sums[...], 0)
    ratios = pltpu.roll(summed, ROWS - 1, 1) / summed
    low, mid, high = (ratios[:, index : index + 1] for index in range(3))
    scale = 1.0 / (low * mid * (high - mid))
    linear = mid * (high - low) * scale
    square = (mid - low) * scale
    linear_ref[...] = jnp.broadcast_to(linear, (1, cells))
    square_ref[...] = jnp.broadcast_to(square, (1, cells))


def body(shape, right_side, conductivity, destination, neighbour, orientation, send_list):
    cells = right_side.shape[1]
    ghost = send_list.shape[1]
    ranks = shape[0] * shape[1]
    forward, backward, columns = tables()
    vmem = pl.BlockSpec(memory_space=pltpu.VMEM)
    dma = pltpu.SemaphoreType.DMA
    operands = (
        right_side,
        conductivity[None],
        destination[None],
        neighbour,
        orientation,
        send_list,
        jnp.asarray(forward),
        jnp.asarray(backward),
        jnp.asarray(columns),
    )
    operands = tuple(pltpu.with_memory_space_constraint(item, pltpu.HBM) for item in operands)
    basis, linear, square = pl.pallas_call(
        functools.partial(kernel, shape),
        out_shape=(
            jax.ShapeDtypeStruct((3, ROWS, cells), F32),
            jax.ShapeDtypeStruct((1, cells), F32),
            jax.ShapeDtypeStruct((1, cells), F32),
        ),
        in_specs=[pl.BlockSpec(memory_space=pltpu.HBM)] * len(operands),
        out_specs=(vmem, vmem, vmem),
        scratch_shapes=[pltpu.VMEM(item.shape, item.dtype) for item in operands]
        + [
            pltpu.VMEM((ROWS, cells), F32),
            pltpu.VMEM((6, cells, cells), BF),
            pltpu.VMEM((2, ghost, cells), BF),
            pltpu.VMEM((2, cells, ghost), BF),
            pltpu.VMEM((2, MOVE, ROWS), F32),
            pltpu.VMEM((2, MOVE, ROWS), F32),
            pltpu.VMEM((2, MOVE // 2, ROWS), F32),
            pltpu.VMEM((2, MOVE // 2, ROWS), F32),
            pltpu.VMEM((2, 2, HALO, ghost), F32),
            pltpu.VMEM((2, 2, HALO, ghost), F32),
            pltpu.VMEM((ranks, 1, ROWS), F32),
            pltpu.VMEM((2 * FACE, cells), F32),
            dma((len(operands),)),
            dma((2,)),
            dma((2,)),
            dma((2,)),
            dma((2,)),
            dma((2, 2)),
            dma((2, 2)),
            dma,
            dma,
        ],
        compiler_params=pltpu.CompilerParams(
            collective_id=0, has_side_effects=True, vmem_limit_bytes=VMEM_LIMIT
        ),
    )(*operands)
    first, second, third = (basis[index, :BLOCK] for index in range(3))
    return linear * first - square * second, first - linear * second + square * third


def solution(mesh):
    both = ("curve", "group")
    shape = (mesh.shape["curve"], mesh.shape["group"])
    in_specs = (P(None, both), P(both), P(both), P(None, both), P(None, both), P(None, both))
    out_specs = (P(None, both), P(None, both))
    return jax.shard_map(
        functools.partial(body, shape),
        mesh=mesh,
        in_specs=in_specs,
        out_specs=out_specs,
        check_vma=False,
    )
```

```python
import functools

import jax
import jax.numpy as jnp
import numpy as np
from jax import lax
from jax.experimental import pallas as pl
from jax.experimental.pallas import tpu as pltpu
from jax.sharding import PartitionSpec as P

NODES = 5
BLOCK = 125
MOVE = 64
UNROLLED = 64
VMEM_LIMIT = 24 * 1024 * 1024
PENALTY = 80.0
MESH = pl.DeviceIdType.MESH
BF = jnp.bfloat16
F32 = jnp.float32

ROWS = 128
KAPPA = 125
TAG = 126
PART = 32
FACE = 2 * PART
FACE_KAPPA = 25
FACE_TAG = 26
HALO = PART + 24
FACE_LAST = 27

GAUSS_POINTS = (-0.906179845938664, -0.5384693101056831, 0.0, 0.5384693101056831, 0.906179845938664)
GAUSS_WEIGHTS = (
    0.2369268850561891,
    0.4786286704993665,
    0.5688888888888889,
    0.4786286704993665,
    0.2369268850561891,
)


def lagrange_value(points, position, location):
    out = 1.0
    for other in range(len(points)):
        if other != position:
            out = out * (location - points[other]) / (points[position] - points[other])
    return out


def lagrange_slope(points, position, location):
    total = 0.0
    for skipped in range(len(points)):
        if skipped == position:
            continue
        addend = 1.0 / (points[position] - points[skipped])
        for other in range(len(points)):
            if other != position and other != skipped:
                addend = addend * (location - points[other]) / (points[position] - points[other])
        total = total + addend
    return total


def along_axis(matrix, axis):
    five = np.eye(NODES)
    plane = np.eye(NODES * NODES)
    if axis == 0:
        return np.kron(matrix, plane)
    if axis == 1:
        return np.kron(five, np.kron(matrix, five))
    return np.kron(plane, matrix)


def split_table(table):
    high = table.astype(BF)
    low = (table - high.astype(np.float64)).astype(BF)
    return high, low


def tables():
    points = [0.5 * (value + 1.0) for value in GAUSS_POINTS]
    weights = np.array([0.5 * value for value in GAUSS_WEIGHTS])
    slopes = np.array([[lagrange_slope(points, p, points[q]) for p in range(NODES)] for q in range(NODES)])
    ends = [np.array([lagrange_value(points, p, at) for p in range(NODES)]) for at in (0.0, 1.0)]
    normals = [
        np.array([sign * lagrange_slope(points, p, at) for p in range(NODES)])
        for sign, at in ((-1.0, 0.0), (1.0, 1.0))
    ]
    cell_weight = np.kron(weights, np.kron(weights, weights))
    stiffness = np.zeros((BLOCK, BLOCK))
    for axis in range(3):
        grad = along_axis(slopes, axis)
        stiffness += grad.T @ (cell_weight[:, None] * grad)
    half = np.sqrt(0.5)
    parity_rows = np.zeros((NODES, NODES))
    for row, (a, b, sign) in enumerate(((0, 4, 1), (1, 3, 1), (2, 2, 1), (0, 4, -1), (1, 3, -1))):
        if a == b:
            parity_rows[row, a] = 1.0
        else:
            parity_rows[row, a] = half
            parity_rows[row, b] = sign * half
    parity = np.array([0, 0, 0, 1, 1])
    row_weight = weights[[0, 1, 2, 0, 1]]
    both = np.kron(parity_rows, parity_rows)
    count = NODES * NODES
    trace = np.zeros((6 * FACE, ROWS))
    for face in range(6):
        start = face * FACE
        trace[start : start + count, :BLOCK] = both @ along_axis(ends[face % 2][None, :], face // 2)
        trace[start + PART : start + PART + count, :BLOCK] = both @ along_axis(
            normals[face % 2][None, :], face // 2
        )
    lift = trace.T.copy()
    for face in range(6):
        trace[face * FACE + FACE_KAPPA, KAPPA] = 1.0
    first = np.zeros((6 * FACE + ROWS, ROWS))
    first[: 6 * FACE] = trace
    first[6 * FACE : 6 * FACE + BLOCK, :BLOCK] = stiffness
    high, low = split_table(first)
    forward = np.concatenate([high, high, low], 1)
    high, low = split_table(lift)
    backward = np.concatenate([high, low], 0)
    columns = np.zeros((ROWS, ROWS), np.float32)
    columns[:BLOCK, 0] = cell_weight
    columns[:count, 1] = np.kron(row_weight, row_weight)
    columns[:count, 2] = 2.0 * np.kron(parity, np.ones(NODES))
    columns[:count, 3] = 2.0 * np.kron(np.ones(NODES), parity)
    return forward, backward, columns


def split_two(value):
    high = value.astype(BF)
    low = (value - high.astype(F32)).astype(BF)
    return high, low


def split_three(value):
    high = value.astype(BF)
    rest = value - high.astype(F32)
    mid = rest.astype(BF)
    return high, mid, (rest - mid.astype(F32)).astype(BF)


def one_hot(left, right):
    return jnp.where(left == right, 1.0, 0.0).astype(BF)


def dot(left, right):
    return jnp.dot(left, right, preferred_element_type=F32)


def dot_last(left, right):
    return lax.dot_general(left, right, (((1,), (1,)), ((), ())), preferred_element_type=F32)


def iota(shape, dim):
    return lax.broadcasted_iota(jnp.int32, shape, dim)


def rounds_of(group):
    rounds, reach = [(1, 2)], 2
    while reach < group - 1:
        rounds.append((reach,))
        reach *= 2
    return rounds


def kernel(
    shape,
    rhs_hbm,
    cond_hbm,
    dest_hbm,
    neigh_hbm,
    orient_hbm,
    list_hbm,
    forward_hbm,
    backward_hbm,
    column_hbm,
    basis,
    linear_ref,
    square_ref,
    rhs_ref,
    cond_ref,
    dest_ref,
    neigh_ref,
    orient_ref,
    list_ref,
    forward_ref,
    backward_ref,
    column_ref,
    payload,
    local_hot,
    ghost_hot,
    send_hot,
    packed,
    moved,
    far_out,
    far_in,
    halo_out,
    halo_in,
    sums,
    kept,
    load_sem,
    move_send,
    move_recv,
    far_send,
    far_recv,
    halo_send,
    halo_recv,
    sum_send,
    sum_recv,
    seen,
):
    curve, group = shape
    ranks = curve * group
    cells = rhs_ref.shape[1]
    ghost = list_ref.shape[1]
    me = lax.axis_index("curve") * group + lax.axis_index("group")

    def place(rank):
        return (rank // group, lax.rem(rank, group))

    def other(step):
        return place(lax.rem(me + step, ranks))

    class Exchange:
        def __init__(self, source, target, send_sem, recv_sem, reach):
            self.there = (me >= reach, me + reach < ranks)
            self.copies = [
                pltpu.make_async_remote_copy(
                    src_ref=source.at[side],
                    dst_ref=target.at[1 - side],
                    send_sem=send_sem.at[side],
                    recv_sem=recv_sem.at[1 - side],
                    device_id=device,
                    device_id_type=MESH,
                )
                for side, device in ((0, other(ranks - reach)), (1, other(reach)))
            ]

        def start(self, side):
            pl.when(self.there[side])(self.copies[side].start)

        def arrive(self, side):
            pl.when(self.there[side])(self.copies[1 - side].wait_recv)

        def leave(self):
            for side in range(2):
                pl.when(self.there[side])(self.copies[side].wait_send)

    def clear(reach, refs):
        for side, missing in ((0, me < reach), (1, me + reach >= ranks)):

            @pl.when(missing)
            def _():
                for ref in refs:
                    ref[side] = jnp.zeros(ref.shape[1:], ref.dtype)

    barrier = pltpu.get_barrier_semaphore()

    my_curve, my_group = lax.axis_index("curve"), lax.axis_index("group")

    def for_each_other(act):
        def one(to_group):
            for step in range(curve):
                to = (lax.rem(my_curve + step, curve), to_group)
                if step:
                    act(to)
                else:
                    pl.when(to_group != my_group)(functools.partial(act, to))

        if ranks <= UNROLLED:
            for to_group in range(group):
                one(to_group)
        else:
            pl.loop(0, group)(one)

    def signal(semaphore, device):
        pl.semaphore_signal(semaphore, inc=1, device_id=device, device_id_type=MESH)

    greeted = curve - 1
    for step in (2, 1):
        for there, device in (
            (me + step < ranks, other(step)),
            (me >= step, other(ranks - step)),
        ):
            pl.when(there)(functools.partial(signal, barrier, device))
            greeted = greeted + there.astype(jnp.int32)
    for step in range(1, curve):
        signal(barrier, (lax.rem(my_curve + step, curve), my_group))

    def spread(index):
        for step in rounds_of(group)[index]:
            for there, to in (
                (my_group + step < group, my_group + step),
                (my_group >= step, my_group - step),
            ):
                pl.when(there)(functools.partial(signal, seen.at[index], (my_curve, to)))

    def gather(index):
        count = 0
        for step in rounds_of(group)[index]:
            count = count + (my_group + step < group).astype(jnp.int32)
            count = count + (my_group >= step).astype(jnp.int32)
        pl.semaphore_wait(seen.at[index], count)

    loads = [
        pltpu.make_async_copy(source, target, load_sem.at[index])
        for index, (source, target) in enumerate(
            (
                (dest_hbm, dest_ref),
                (list_hbm, list_ref),
                (cond_hbm, cond_ref),
                (rhs_hbm, rhs_ref),
                (forward_hbm, forward_ref),
                (neigh_hbm, neigh_ref),
                (orient_hbm, orient_ref),
                (column_hbm, column_ref),
                (backward_hbm, backward_ref),
            )
        )
    ]
    for load in loads:
        load.start()
    clear(1, (moved, halo_in.at[0], halo_in.at[1]))
    clear(2, (far_in,))
    for load in loads[:4]:
        load.wait()

    def faces_of(stacked, kappa, first, last):
        part = dot(forward_ref[first * FACE : last * FACE, :], stacked)
        own, halves = [], []
        for index in range(last - first):
            value = part[index * FACE : index * FACE + PART]
            flux = kappa * part[index * FACE + PART : (index + 1) * FACE]
            own.append((value, flux))
            halves.append(jnp.concatenate(split_two(jnp.concatenate([value, flux], 0)), 0))
        return own, halves

    offset = dest_ref[...] - me * cells
    goes_left = offset < 0
    goes_right = offset >= cells
    slot = jnp.where(goes_left, offset + cells, jnp.where(goes_right, offset - cells, offset))
    payload[0:BLOCK, :] = rhs_ref[...]
    payload[KAPPA : KAPPA + 1, :] = cond_ref[...]
    payload[TAG : TAG + 1, :] = (slot + 1).astype(F32)
    payload[TAG + 1 : TAG + 2, :] = jnp.zeros((1, cells), F32)
    high, mid, low = split_three(payload[...])
    parts = jnp.concatenate([high, mid, low], 0)
    row8 = iota((8, cells), 0)
    leaving = jnp.where(
        row8 == 0,
        jnp.where(goes_left, 1.0, 0.0),
        jnp.where(row8 == 1, jnp.where(goes_right, 1.0, 0.0), 0.0),
    ).astype(BF)
    triangle = jnp.where(iota((cells, cells), 0) <= iota((cells, cells), 1), 1.0, 0.0).astype(BF)
    order = dot(leaving, triangle).astype(jnp.int32) - 1
    slots = iota((MOVE, cells), 0)
    pick = jnp.concatenate(
        [
            one_hot(jnp.where(goes_left, order[0:1], -1), slots),
            one_hot(jnp.where(goes_right, order[1:2], -1), slots),
        ],
        0,
    )
    chosen = dot_last(pick, parts)
    chosen = chosen[:, :ROWS] + chosen[:, ROWS : 2 * ROWS] + chosen[:, 2 * ROWS :]
    packed[0] = chosen[:MOVE]
    packed[1] = chosen[MOVE:]

    pl.semaphore_wait(barrier, greeted)

    moves = Exchange(packed, moved, move_send, move_recv, 1)
    for side in range(2):
        moves.start(side)

    for load in loads[4:]:
        load.wait()

    old_halves = faces_of(jnp.concatenate([high, mid, high], 0), cond_ref[...], 0, 2)[1]
    offset_column = jnp.broadcast_to(offset.astype(F32), (8, cells)).T[:, 0:1]
    lists = list_ref[...].astype(F32)
    halo_rows = iota((HALO, ghost), 0)

    def shrink(out):
        out = out[:FACE] + out[FACE:]
        return jnp.where(halo_rows == FACE_LAST, out[HALO : HALO + 1], out[:HALO])

    def widen(message):
        last = message[FACE_LAST : FACE_LAST + 1]
        rest = jnp.where(iota((FACE - HALO, ghost), 0) == 0, last, 0.0)
        return jnp.concatenate([message, rest], 0)

    for side in range(2):
        hot = one_hot(offset_column, lists[side : side + 1, :])
        out = dot(old_halves[side], hot)
        halo_out[0, side] = jnp.where(
            halo_rows == FACE_TAG, lists[side : side + 1, :], shrink(out)
        )
    lanes = iota((2 * MOVE, ROWS), 1)
    tagged = jnp.where(lanes == FACE_TAG, chosen[:, TAG : TAG + 1], 0.0)
    leaving_low = dot_last(pick, old_halves[0]) + tagged
    leaving_high = dot_last(pick, old_halves[1]) + tagged
    leaving_low = leaving_low[:, :FACE] + leaving_low[:, FACE:]
    leaving_high = leaving_high[:, :FACE] + leaving_high[:, FACE:]
    middle = MOVE // 2
    far_out[0] = jnp.concatenate([leaving_low[:middle], leaving_low[middle:MOVE]], 1)
    far_out[1] = jnp.concatenate([leaving_high[MOVE : MOVE + middle], leaving_high[MOVE + middle :]], 1)

    halos = Exchange(halo_out.at[0], halo_in.at[0], halo_send.at[0], halo_recv.at[0], 1)
    fars = Exchange(far_out, far_in, far_send, far_recv, 2)
    for copies in (fars, halos):
        for side in range(2):
            copies.start(side)
    spread(0)

    stay = one_hot(iota((cells, cells), 0), offset)
    arrived = dot_last(parts, stay)
    cell_rows = iota((cells, cells), 0)
    ghost_rows = iota((ghost, cells), 0)
    for face in range(6):
        local_hot[face] = one_hot(neigh_ref[face : face + 1, :], cell_rows)
    for side in range(2):
        ghost_hot[side] = one_hot(
            neigh_ref[side : side + 1, :] - (cells + side * ghost), ghost_rows
        )
        send_hot[side] = one_hot(list_ref[side : side + 1, :], iota((cells, ghost), 0))

    for side in range(2):
        moves.arrive(side)
    record = moved[...].reshape(2 * MOVE, ROWS)
    landing = record[:, TAG : TAG + 1].astype(jnp.int32) - 1
    record_parts = jnp.concatenate(split_three(record.T), 0)
    arrived = arrived + dot(record_parts, one_hot(landing, iota((2 * MOVE, cells), 1)))
    arrived = arrived[:ROWS] + arrived[ROWS : 2 * ROWS] + arrived[2 * ROWS :]
    rows = iota((ROWS, cells), 0)
    field = jnp.where(rows < BLOCK, arrived, 0.0)
    kappa = arrived[KAPPA : KAPPA + 1]
    cell_weight = column_ref[:, 0:1]
    face_weight = column_ref[0:PART, 1:2]
    first_odd = column_ref[0:PART, 2:3]
    second_odd = column_ref[0:PART, 3:4]

    def signs(face):
        code = orient_ref[face : face + 1, :]
        first_bit = jnp.where(lax.rem(code, 2) == 1, 1.0, 0.0)
        second_bit = jnp.where(code >= 2, 1.0, 0.0)
        return (1.0 - first_odd * first_bit) * (1.0 - second_odd * second_bit)

    def outer(face):
        return jnp.where(neigh_ref[face : face + 1, :] < 0, 1.0, 0.0)

    def coefficients(face, own, near):
        value, flux = own
        sign = signs(face)
        outside = outer(face)
        near = near[:FACE] + near[FACE:]
        near_kappa = near[FACE_KAPPA : FACE_KAPPA + 1] + outside * kappa
        penalty = PENALTY * jnp.maximum(kappa, near_kappa)
        jump = value - (sign * near[:PART] - outside * value)
        mean = flux - (sign * near[PART:] - outside * flux)
        scaled = -0.5 * (face_weight * jump)
        first = face_weight * (penalty * jump - 0.5 * mean)
        return (first, kappa * scaled), (jump, mean, first, scaled)

    def lifted(terms, first, last):
        high, low = split_two(jnp.concatenate(terms, 0))
        both = dot(backward_ref[:, first * FACE : last * FACE], high)
        rest = dot(backward_ref[0:ROWS, first * FACE : last * FACE], low)
        return both[:ROWS] + both[ROWS:] + rest

    def stack(field):
        high, low = split_two(jnp.where(rows == KAPPA, kappa, field))
        return jnp.concatenate([high, low, high], 0)

    def inner(field, stacked, halves):
        more_own, more_halves = faces_of(stacked, kappa, 2, 6)
        terms = []
        for face in range(2, 6):
            near = dot(more_halves[(face ^ 1) - 2], local_hot[face])
            terms += coefficients(face, more_own[face - 2], near)[0]
        result = lifted(terms, 2, 6)
        stiff = dot(forward_ref[6 * FACE :, :], stacked)
        result = result + cell_weight * field + kappa * stiff
        return result, [dot(halves[face ^ 1], local_hot[face]) for face in range(2)]

    def with_ghosts(near, ghosts, side):
        return near + dot(jnp.concatenate(split_two(ghosts), 0), ghost_hot[side])

    def down(value):
        return jnp.sum(value, 0, keepdims=True)

    def across(value):
        return jnp.sum(value, 1, keepdims=True)

    basis[0] = field
    stacked = stack(field)
    own, halves = faces_of(stacked, kappa, 0, 2)
    result, near = inner(field, stacked, halves)
    for side in range(2):
        halos.arrive(side)
        fars.arrive(side)
    gather(0)
    terms = []
    for face in range(2):
        ghosts = widen(halo_in[0, face])
        gone = leaving_high[:MOVE] if face == 0 else leaving_low[MOVE:]
        far = far_in[face]
        wide = jnp.concatenate([far[:, :FACE], far[:, FACE:], gone], 0)
        hot = one_hot(wide[:, FACE_TAG : FACE_TAG + 1] - 1.0, ghosts[FACE_TAG : FACE_TAG + 1])
        placed = dot(jnp.concatenate(split_two(wide.T), 0), hot)
        ghosts = ghosts + placed[:FACE] + placed[FACE:]
        terms += coefficients(face, own[face], with_ghosts(near[face], ghosts, face))[0]
    image = result + lifted(terms, 0, 2)

    stacked = stack(image)
    images = Exchange(halo_out.at[1], halo_in.at[1], halo_send.at[1], halo_recv.at[1], 1)
    own_right, halves_right = faces_of(stacked, kappa, 1, 2)
    halo_out[1, 1] = shrink(dot(halves_right[0], send_hot[1]))
    images.start(1)
    if len(rounds_of(group)) > 1:
        spread(1)
    basis[1] = image
    own_left, halves_left = faces_of(stacked, kappa, 0, 1)
    own, halves = own_left + own_right, halves_left + halves_right
    result, near = inner(image, stacked, halves)
    halo_out[1, 0] = shrink(dot(halves[0], send_hot[0]))
    images.start(0)
    value, flux = own[1]
    edge = 2.0 * outer(1) * down(face_weight * (value * (PENALTY * kappa * value - flux)))
    found = [across(down(field * field)), across(down(field * image)), across(down(image * image))]
    outside = outer(0) > 0.0
    kept[...] = near[0]
    _, (jump, mean, first, scaled) = coefficients(0, own[0], near[0])

    inside = jnp.where(outside, own[0][0], jump) * first + jnp.where(outside, own[0][1], mean) * scaled
    inside = jnp.where(neigh_ref[0:1, :] < cells, down(inside), 0.0)
    found.append(across(down(image * result) + edge + inside))
    lane = iota((1, ROWS), 1)
    message = jnp.zeros((1, ROWS), F32)
    for index, value in enumerate(found):
        message = jnp.where(lane == index, value, message)
    across_edge = dot_last(halves[0], ghost_hot[0])
    across_edge = across_edge[:FACE] + across_edge[FACE:]
    code = orient_ref[0:1, :]
    bit_rows = iota((8, cells), 0)
    bits = jnp.where(
        bit_rows == 0, lax.rem(code, 2), jnp.where(bit_rows == 1, jnp.where(code >= 2, 1, 0), 1)
    )
    bits = dot_last(bits.astype(F32).astype(BF), ghost_hot[0])
    slot_sign = (1.0 - first_odd * bits[0:1]) * (1.0 - second_odd * bits[1:2])
    slot_weight = face_weight * bits[2:3]
    slot_kappa = across_edge[FACE_KAPPA : FACE_KAPPA + 1]

    for index in range(1, len(rounds_of(group))):
        if index > 1:
            spread(index)
        if index < len(rounds_of(group)) - 1:
            gather(index)
    images.arrive(0)
    if len(rounds_of(group)) > 1:
        gather(len(rounds_of(group)) - 1)
    ghosts = widen(halo_in[1, 0])
    penalty = PENALTY * jnp.maximum(slot_kappa, ghosts[FACE_KAPPA : FACE_KAPPA + 1])
    jump = across_edge[:PART] - slot_sign * ghosts[:PART]
    mean = across_edge[PART:] - slot_sign * ghosts[PART:]
    shared = across(down(slot_weight * (jump * (penalty * jump - mean))))
    sums[me] = message + jnp.where(lane == 3, shared, 0.0)

    for_each_other(
        lambda device: pltpu.make_async_remote_copy(
            src_ref=sums.at[me],
            dst_ref=sums.at[me],
            send_sem=sum_send,
            recv_sem=sum_recv,
            device_id=device,
            device_id_type=MESH,
        ).start()
    )

    images.arrive(1)
    terms = []
    near[0] = kept[...]
    for face in range(2):
        terms += coefficients(face, own[face], with_ghosts(near[face], widen(halo_in[1, face]), face))[0]
    basis[2] = result + lifted(terms, 0, 2)
    for copies in (moves, halos, fars, images):
        copies.leave()
    rest = sums.at[pl.ds(1, ranks - 1)]
    pltpu.make_async_copy(rest, rest, sum_send).wait()
    pltpu.make_async_copy(rest, rest, sum_recv).wait()
    summed = jnp.sum(sums[...], 0)
    ratios = pltpu.roll(summed, ROWS - 1, 1) / summed
    low, mid, high = (ratios[:, index : index + 1] for index in range(3))
    scale = 1.0 / (low * mid * (high - mid))
    linear = mid * (high - low) * scale
    square = (mid - low) * scale
    linear_ref[...] = jnp.broadcast_to(linear, (1, cells))
    square_ref[...] = jnp.broadcast_to(square, (1, cells))


def body(shape, right_side, conductivity, destination, neighbour, orientation, send_list):
    cells = right_side.shape[1]
    ghost = send_list.shape[1]
    ranks = shape[0] * shape[1]
    forward, backward, columns = tables()
    vmem = pl.BlockSpec(memory_space=pltpu.VMEM)
    dma = pltpu.SemaphoreType.DMA
    operands = (
        right_side,
        conductivity[None],
        destination[None],
        neighbour,
        orientation,
        send_list,
        jnp.asarray(forward),
        jnp.asarray(backward),
        jnp.asarray(columns),
    )
    operands = tuple(pltpu.with_memory_space_constraint(item, pltpu.HBM) for item in operands)
    basis, linear, square = pl.pallas_call(
        functools.partial(kernel, shape),
        out_shape=(
            jax.ShapeDtypeStruct((3, ROWS, cells), F32),
            jax.ShapeDtypeStruct((1, cells), F32),
            jax.ShapeDtypeStruct((1, cells), F32),
        ),
        in_specs=[pl.BlockSpec(memory_space=pltpu.HBM)] * len(operands),
        out_specs=(vmem, vmem, vmem),
        scratch_shapes=[pltpu.VMEM(item.shape, item.dtype) for item in operands]
        + [
            pltpu.VMEM((ROWS, cells), F32),
            pltpu.VMEM((6, cells, cells), BF),
            pltpu.VMEM((2, ghost, cells), BF),
            pltpu.VMEM((2, cells, ghost), BF),
            pltpu.VMEM((2, MOVE, ROWS), F32),
            pltpu.VMEM((2, MOVE, ROWS), F32),
            pltpu.VMEM((2, MOVE // 2, ROWS), F32),
            pltpu.VMEM((2, MOVE // 2, ROWS), F32),
            pltpu.VMEM((2, 2, HALO, ghost), F32),
            pltpu.VMEM((2, 2, HALO, ghost), F32),
            pltpu.VMEM((ranks, 1, ROWS), F32),
            pltpu.VMEM((2 * FACE, cells), F32),
            dma((len(operands),)),
            dma((2,)),
            dma((2,)),
            dma((2,)),
            dma((2,)),
            dma((2, 2)),
            dma((2, 2)),
            dma,
            dma,
            pltpu.SemaphoreType.REGULAR((len(rounds_of(shape[1])),)),
        ],
        compiler_params=pltpu.CompilerParams(
            collective_id=0, has_side_effects=True, vmem_limit_bytes=VMEM_LIMIT
        ),
    )(*operands)
    first, second, third = (basis[index, :BLOCK] for index in range(3))
    return linear * first - square * second, first - linear * second + square * third


def solution(mesh):
    both = ("curve", "group")
    shape = (mesh.shape["curve"], mesh.shape["group"])
    in_specs = (P(None, both), P(both), P(both), P(None, both), P(None, both), P(None, both))
    out_specs = (P(None, both), P(None, both))
    return jax.shard_map(
        functools.partial(body, shape),
        mesh=mesh,
        in_specs=in_specs,
        out_specs=out_specs,
        check_vma=False,
    )
```

```python
import functools

import jax
import jax.numpy as jnp
import numpy as np
from jax import lax
from jax.experimental import pallas as pl
from jax.experimental.pallas import tpu as pltpu
from jax.sharding import PartitionSpec as P

NODES = 5
BLOCK = 125
MOVE = 64
UNROLLED = 64
VMEM_LIMIT = 24 * 1024 * 1024
PENALTY = 80.0
MESH = pl.DeviceIdType.MESH
BF = jnp.bfloat16
F32 = jnp.float32

ROWS = 128
KAPPA = 125
TAG = 126
PART = 32
FACE = 2 * PART
FACE_KAPPA = 25
FACE_TAG = 26
HALO = PART + 24
FACE_LAST = 27

GAUSS_POINTS = (-0.906179845938664, -0.5384693101056831, 0.0, 0.5384693101056831, 0.906179845938664)
GAUSS_WEIGHTS = (
    0.2369268850561891,
    0.4786286704993665,
    0.5688888888888889,
    0.4786286704993665,
    0.2369268850561891,
)


def lagrange_value(points, position, location):
    out = 1.0
    for other in range(len(points)):
        if other != position:
            out = out * (location - points[other]) / (points[position] - points[other])
    return out


def lagrange_slope(points, position, location):
    total = 0.0
    for skipped in range(len(points)):
        if skipped == position:
            continue
        addend = 1.0 / (points[position] - points[skipped])
        for other in range(len(points)):
            if other != position and other != skipped:
                addend = addend * (location - points[other]) / (points[position] - points[other])
        total = total + addend
    return total


def along_axis(matrix, axis):
    five = np.eye(NODES)
    plane = np.eye(NODES * NODES)
    if axis == 0:
        return np.kron(matrix, plane)
    if axis == 1:
        return np.kron(five, np.kron(matrix, five))
    return np.kron(plane, matrix)


def split_table(table):
    high = table.astype(BF)
    low = (table - high.astype(np.float64)).astype(BF)
    return high, low


def tables():
    points = [0.5 * (value + 1.0) for value in GAUSS_POINTS]
    weights = np.array([0.5 * value for value in GAUSS_WEIGHTS])
    slopes = np.array([[lagrange_slope(points, p, points[q]) for p in range(NODES)] for q in range(NODES)])
    ends = [np.array([lagrange_value(points, p, at) for p in range(NODES)]) for at in (0.0, 1.0)]
    normals = [
        np.array([sign * lagrange_slope(points, p, at) for p in range(NODES)])
        for sign, at in ((-1.0, 0.0), (1.0, 1.0))
    ]
    cell_weight = np.kron(weights, np.kron(weights, weights))
    stiffness = np.zeros((BLOCK, BLOCK))
    for axis in range(3):
        grad = along_axis(slopes, axis)
        stiffness += grad.T @ (cell_weight[:, None] * grad)
    half = np.sqrt(0.5)
    parity_rows = np.zeros((NODES, NODES))
    for row, (a, b, sign) in enumerate(((0, 4, 1), (1, 3, 1), (2, 2, 1), (0, 4, -1), (1, 3, -1))):
        if a == b:
            parity_rows[row, a] = 1.0
        else:
            parity_rows[row, a] = half
            parity_rows[row, b] = sign * half
    parity = np.array([0, 0, 0, 1, 1])
    row_weight = weights[[0, 1, 2, 0, 1]]
    both = np.kron(parity_rows, parity_rows)
    count = NODES * NODES
    trace = np.zeros((6 * FACE, ROWS))
    for face in range(6):
        start = face * FACE
        trace[start : start + count, :BLOCK] = both @ along_axis(ends[face % 2][None, :], face // 2)
        trace[start + PART : start + PART + count, :BLOCK] = both @ along_axis(
            normals[face % 2][None, :], face // 2
        )
    lift = trace.T.copy()
    right = trace[FACE : 2 * FACE].copy()
    for face in range(6):
        trace[face * FACE + FACE_KAPPA, KAPPA] = 1.0
    first = np.zeros((6 * FACE + 2 * ROWS, ROWS))
    first[: 6 * FACE] = trace
    first[6 * FACE : 6 * FACE + BLOCK, :BLOCK] = stiffness
    first[6 * FACE + ROWS : 7 * FACE + ROWS, :BLOCK] = right[:, :BLOCK] @ stiffness
    first[7 * FACE + ROWS :, :BLOCK] = right[:, :BLOCK] * cell_weight
    high, low = split_table(first)
    forward = np.concatenate([high, high, low], 1)
    backward = np.concatenate(split_table(lift) + split_table(right @ lift), 0)
    columns = np.zeros((ROWS, ROWS), np.float32)
    columns[:BLOCK, 0] = cell_weight
    columns[:count, 1] = np.kron(row_weight, row_weight)
    columns[:count, 2] = 2.0 * np.kron(parity, np.ones(NODES))
    columns[:count, 3] = 2.0 * np.kron(np.ones(NODES), parity)
    return forward, backward, columns


def split_two(value):
    high = value.astype(BF)
    low = (value - high.astype(F32)).astype(BF)
    return high, low


def split_three(value):
    high = value.astype(BF)
    rest = value - high.astype(F32)
    mid = rest.astype(BF)
    return high, mid, (rest - mid.astype(F32)).astype(BF)


def one_hot(left, right):
    return jnp.where(left == right, 1.0, 0.0).astype(BF)


def dot(left, right):
    return jnp.dot(left, right, preferred_element_type=F32)


def dot_last(left, right):
    return lax.dot_general(left, right, (((1,), (1,)), ((), ())), preferred_element_type=F32)


def iota(shape, dim):
    return lax.broadcasted_iota(jnp.int32, shape, dim)


def rounds_of(group):
    rounds, reach = [(1, 2)], 2
    while reach < group - 1:
        rounds.append((reach,))
        reach *= 2
    return rounds


def kernel(
    shape,
    rhs_hbm,
    cond_hbm,
    dest_hbm,
    neigh_hbm,
    orient_hbm,
    list_hbm,
    forward_hbm,
    backward_hbm,
    column_hbm,
    basis,
    linear_ref,
    square_ref,
    rhs_ref,
    cond_ref,
    dest_ref,
    neigh_ref,
    orient_ref,
    list_ref,
    forward_ref,
    backward_ref,
    column_ref,
    payload,
    local_hot,
    ghost_hot,
    send_hot,
    packed,
    moved,
    far_out,
    far_in,
    halo_out,
    halo_in,
    sums,
    kept,
    near_ref,
    tag_out,
    tag_in,
    tag_send,
    tag_recv,
    load_sem,
    move_send,
    move_recv,
    far_send,
    far_recv,
    halo_send,
    halo_recv,
    sum_send,
    sum_recv,
    seen,
):
    curve, group = shape
    ranks = curve * group
    cells = rhs_ref.shape[1]
    ghost = list_ref.shape[1]
    me = lax.axis_index("curve") * group + lax.axis_index("group")

    def place(rank):
        return (rank // group, lax.rem(rank, group))

    def other(step):
        return place(lax.rem(me + step, ranks))

    class Exchange:
        def __init__(self, source, target, send_sem, recv_sem, reach):
            self.there = (me >= reach, me + reach < ranks)
            self.copies = [
                pltpu.make_async_remote_copy(
                    src_ref=source.at[side],
                    dst_ref=target.at[1 - side],
                    send_sem=send_sem.at[side],
                    recv_sem=recv_sem.at[1 - side],
                    device_id=device,
                    device_id_type=MESH,
                )
                for side, device in ((0, other(ranks - reach)), (1, other(reach)))
            ]

        def start(self, side):
            pl.when(self.there[side])(self.copies[side].start)

        def arrive(self, side):
            pl.when(self.there[side])(self.copies[1 - side].wait_recv)

        def leave(self):
            for side in range(2):
                pl.when(self.there[side])(self.copies[side].wait_send)

    def clear(reach, refs):
        for side, missing in ((0, me < reach), (1, me + reach >= ranks)):

            @pl.when(missing)
            def _():
                for ref in refs:
                    ref[side] = jnp.zeros(ref.shape[1:], ref.dtype)

    barrier = pltpu.get_barrier_semaphore()

    my_curve, my_group = lax.axis_index("curve"), lax.axis_index("group")

    def for_each_other(act):
        def one(to_group):
            for step in range(curve):
                to = (lax.rem(my_curve + step, curve), to_group)
                if step:
                    act(to)
                else:
                    pl.when(to_group != my_group)(functools.partial(act, to))

        if ranks <= UNROLLED:
            for to_group in range(group):
                one(to_group)
        else:
            pl.loop(0, group)(one)

    def signal(semaphore, device):
        pl.semaphore_signal(semaphore, inc=1, device_id=device, device_id_type=MESH)

    greeted = curve - 1
    for step in (2, 1):
        for there, device in (
            (me + step < ranks, other(step)),
            (me >= step, other(ranks - step)),
        ):
            pl.when(there)(functools.partial(signal, barrier, device))
            greeted = greeted + there.astype(jnp.int32)
    for step in range(1, curve):
        signal(barrier, (lax.rem(my_curve + step, curve), my_group))

    def spread(index):
        for step in rounds_of(group)[index]:
            for there, to in (
                (my_group + step < group, my_group + step),
                (my_group >= step, my_group - step),
            ):
                pl.when(there)(functools.partial(signal, seen.at[index], (my_curve, to)))

    def gather(index):
        count = 0
        for step in rounds_of(group)[index]:
            count = count + (my_group + step < group).astype(jnp.int32)
            count = count + (my_group >= step).astype(jnp.int32)
        pl.semaphore_wait(seen.at[index], count)

    loads = [
        pltpu.make_async_copy(source, target, load_sem.at[index])
        for index, (source, target) in enumerate(
            (
                (dest_hbm, dest_ref),
                (list_hbm, list_ref),
                (cond_hbm, cond_ref),
                (rhs_hbm, rhs_ref),
                (forward_hbm, forward_ref),
                (neigh_hbm, neigh_ref),
                (orient_hbm, orient_ref),
                (column_hbm, column_ref),
                (backward_hbm, backward_ref),
            )
        )
    ]
    for load in loads:
        load.start()
    clear(1, (moved, tag_in, halo_in.at[0], halo_in.at[1]))
    clear(2, (far_in,))
    for load in loads[:4]:
        load.wait()

    def faces_of(stacked, kappa, first, last):
        part = dot(forward_ref[first * FACE : last * FACE, :], stacked)
        own, halves = [], []
        for index in range(last - first):
            value = part[index * FACE : index * FACE + PART]
            flux = kappa * part[index * FACE + PART : (index + 1) * FACE]
            own.append((value, flux))
            halves.append(jnp.concatenate(split_two(jnp.concatenate([value, flux], 0)), 0))
        return own, halves

    offset = dest_ref[...] - me * cells
    goes_left = offset < 0
    goes_right = offset >= cells
    slot = jnp.where(goes_left, offset + cells, jnp.where(goes_right, offset - cells, offset))
    payload[0:BLOCK, :] = rhs_ref[...]
    payload[KAPPA : KAPPA + 1, :] = cond_ref[...]
    payload[TAG : TAG + 1, :] = (slot + 1).astype(F32)
    payload[TAG + 1 : TAG + 2, :] = jnp.zeros((1, cells), F32)
    high, mid, low = split_three(payload[...])
    parts = jnp.concatenate([high, mid, low], 0)
    row8 = iota((8, cells), 0)
    leaving = jnp.where(
        row8 == 0,
        jnp.where(goes_left, 1.0, 0.0),
        jnp.where(row8 == 1, jnp.where(goes_right, 1.0, 0.0), 0.0),
    ).astype(BF)
    triangle = jnp.where(iota((cells, cells), 0) <= iota((cells, cells), 1), 1.0, 0.0).astype(BF)
    order = dot(leaving, triangle).astype(jnp.int32) - 1
    slots = iota((MOVE, cells), 0)
    pick = jnp.concatenate(
        [
            one_hot(jnp.where(goes_left, order[0:1], -1), slots),
            one_hot(jnp.where(goes_right, order[1:2], -1), slots),
        ],
        0,
    )
    chosen = dot_last(pick, parts)
    chosen = chosen[:, :ROWS] + chosen[:, ROWS : 2 * ROWS] + chosen[:, 2 * ROWS :]
    packed[0] = chosen[:MOVE]
    packed[1] = chosen[MOVE:]

    lists = list_ref[...].astype(F32)
    for side in range(2):
        tag_out[side] = lists[side : side + 1, :]

    pl.semaphore_wait(barrier, greeted)

    moves = Exchange(packed, moved, move_send, move_recv, 1)
    tags = Exchange(tag_out, tag_in, tag_send, tag_recv, 1)
    for copies in (moves, tags):
        for side in range(2):
            copies.start(side)

    for load in loads[4:]:
        load.wait()

    old_halves = faces_of(jnp.concatenate([high, mid, high], 0), cond_ref[...], 0, 2)[1]
    offset_column = jnp.broadcast_to(offset.astype(F32), (8, cells)).T[:, 0:1]
    halo_rows = iota((HALO, ghost), 0)

    def shrink(out):
        out = out[:FACE] + out[FACE:]
        return jnp.where(halo_rows == FACE_LAST, out[HALO : HALO + 1], out[:HALO])

    def widen(message):
        last = message[FACE_LAST : FACE_LAST + 1]
        rest = jnp.where(iota((FACE - HALO, ghost), 0) == 0, last, 0.0)
        return jnp.concatenate([message, rest], 0)

    for side in range(2):
        hot = one_hot(offset_column, lists[side : side + 1, :])
        out = dot(old_halves[side], hot)
        halo_out[0, side] = shrink(out)
    lanes = iota((2 * MOVE, ROWS), 1)
    tagged = jnp.where(lanes == FACE_TAG, chosen[:, TAG : TAG + 1], 0.0)
    leaving_low = dot_last(pick, old_halves[0]) + tagged
    leaving_high = dot_last(pick, old_halves[1]) + tagged
    leaving_low = leaving_low[:, :FACE] + leaving_low[:, FACE:]
    leaving_high = leaving_high[:, :FACE] + leaving_high[:, FACE:]
    middle = MOVE // 2
    far_out[0] = jnp.concatenate([leaving_low[:middle], leaving_low[middle:MOVE]], 1)
    far_out[1] = jnp.concatenate([leaving_high[MOVE : MOVE + middle], leaving_high[MOVE + middle :]], 1)

    halos = Exchange(halo_out.at[0], halo_in.at[0], halo_send.at[0], halo_recv.at[0], 1)
    fars = Exchange(far_out, far_in, far_send, far_recv, 2)
    for copies in (fars, halos):
        for side in range(2):
            copies.start(side)
    spread(0)

    stay = one_hot(iota((cells, cells), 0), offset)
    arrived = dot_last(parts, stay)
    cell_rows = iota((cells, cells), 0)
    ghost_rows = iota((ghost, cells), 0)
    for face in range(6):
        local_hot[face] = one_hot(neigh_ref[face : face + 1, :], cell_rows)
    for side in range(2):
        ghost_hot[side] = one_hot(
            neigh_ref[side : side + 1, :] - (cells + side * ghost), ghost_rows
        )
        send_hot[side] = one_hot(list_ref[side : side + 1, :], iota((cells, ghost), 0))

    def folded(value):
        half = value.shape[0] // 2
        return value[:half] + value[half:]

    arrived = arrived[:ROWS] + arrived[ROWS : 2 * ROWS] + arrived[2 * ROWS :]
    high, low = split_two(arrived)
    stay_halves = faces_of(
        jnp.concatenate([high, low, high], 0), arrived[KAPPA : KAPPA + 1], 0, 6
    )[1]
    for face in range(6):
        near_ref[face] = folded(dot(stay_halves[face ^ 1], local_hot[face]))
    payload[...] = arrived

    for side in range(2):
        moves.arrive(side)
        tags.arrive(side)
    record = moved[...].reshape(2 * MOVE, ROWS)
    landing = record[:, TAG : TAG + 1].astype(jnp.int32) - 1
    record = record.T
    high, mid, low = split_three(record)
    placed = dot(
        jnp.concatenate([high, mid, low], 0), one_hot(landing, iota((2 * MOVE, cells), 1))
    )
    arrived = payload[...] + (placed[:ROWS] + placed[ROWS : 2 * ROWS] + placed[2 * ROWS :])
    moved_halves = faces_of(
        jnp.concatenate([high, mid, high], 0), record[KAPPA : KAPPA + 1], 0, 6
    )[1]
    landing = jnp.where(landing < 0, -2, landing)

    def near_old(face):
        hot = one_hot(landing, neigh_ref[face : face + 1, :])
        return near_ref[face] + folded(dot(moved_halves[face ^ 1], hot))

    rows = iota((ROWS, cells), 0)
    field = jnp.where(rows < BLOCK, arrived, 0.0)
    kappa = arrived[KAPPA : KAPPA + 1]
    cell_weight = column_ref[:, 0:1]
    face_weight = column_ref[0:PART, 1:2]
    first_odd = column_ref[0:PART, 2:3]
    second_odd = column_ref[0:PART, 3:4]

    def signs(face):
        code = orient_ref[face : face + 1, :]
        first_bit = jnp.where(lax.rem(code, 2) == 1, 1.0, 0.0)
        second_bit = jnp.where(code >= 2, 1.0, 0.0)
        return (1.0 - first_odd * first_bit) * (1.0 - second_odd * second_bit)

    def outer(face):
        return jnp.where(neigh_ref[face : face + 1, :] < 0, 1.0, 0.0)

    def coefficients(face, own, near):
        value, flux = own
        sign = signs(face)
        outside = outer(face)
        near_kappa = near[FACE_KAPPA : FACE_KAPPA + 1] + outside * kappa
        penalty = PENALTY * jnp.maximum(kappa, near_kappa)
        jump = value - (sign * near[:PART] - outside * value)
        mean = flux - (sign * near[PART:] - outside * flux)
        scaled = -0.5 * (face_weight * jump)
        first = face_weight * (penalty * jump - 0.5 * mean)
        return (first, kappa * scaled), (jump, mean, first, scaled)

    def lifted(parts, first, last):
        high, low = parts
        both = dot(backward_ref[0 : 2 * ROWS, first * FACE : last * FACE], high)
        rest = dot(backward_ref[0:ROWS, first * FACE : last * FACE], low)
        return both[:ROWS] + both[ROWS:] + rest

    def traced(parts, first, last):
        high, low = parts
        both = dot(backward_ref[2 * ROWS :, first * FACE : last * FACE], high)
        rest = dot(backward_ref[2 * ROWS : 2 * ROWS + FACE, first * FACE : last * FACE], low)
        return both[:FACE] + both[FACE:] + rest

    def split_terms(terms):
        return split_two(jnp.concatenate(terms, 0))

    def stack(field):
        high, low = split_two(jnp.where(rows == KAPPA, kappa, field))
        return jnp.concatenate([high, low, high], 0)

    def inner(field, stacked, own, near):
        terms = []
        for face in range(2, 6):
            terms += coefficients(face, own[face], near(face))[0]
        stiff = dot(forward_ref[6 * FACE : 6 * FACE + ROWS, :], stacked)
        terms = split_terms(terms)
        result = lifted(terms, 2, 6) + cell_weight * field + kappa * stiff
        return result, [near(face) for face in range(2)], terms

    def with_ghosts(near, ghosts, side):
        return near + folded(dot(jnp.concatenate(split_two(ghosts), 0), ghost_hot[side]))

    def down(value):
        return jnp.sum(value, 0, keepdims=True)

    def across(value):
        return jnp.sum(value, 1, keepdims=True)

    basis[0] = field
    stacked = stack(field)
    own = faces_of(stacked, kappa, 0, 6)[0]
    result, near, terms = inner(field, stacked, own, near_old)
    volume = dot(forward_ref[6 * FACE + ROWS :, :], stacked)
    trace = traced(terms, 2, 6) + kappa * volume[:FACE] + volume[FACE:]
    marks = []
    for side in range(2):
        mark = jnp.concatenate(split_two(jnp.broadcast_to(tag_in[side] + 1.0, (8, ghost))), 0)
        mark = dot(mark, ghost_hot[side])
        mark = mark[0:1] + mark[8:9]
        marks.append(jnp.where(mark == 0.0, -1.0, mark))
    for side in range(2):
        halos.arrive(side)
        fars.arrive(side)
    gather(0)
    terms = []
    for face in range(2):
        gone = leaving_high[:MOVE] if face == 0 else leaving_low[MOVE:]
        far = far_in[face]
        wide = jnp.concatenate([far[:, :FACE], far[:, FACE:], gone], 0)
        hot = one_hot(wide[:, FACE_TAG : FACE_TAG + 1], marks[face])
        placed = dot(jnp.concatenate(split_two(wide.T), 0), hot)
        ghosts = with_ghosts(near[face], widen(halo_in[0, face]), face) + folded(placed)
        terms += coefficients(face, own[face], ghosts)[0]
    terms = split_terms(terms)
    trace = trace + traced(terms, 0, 2)
    value = jnp.where(iota((PART, cells), 0) == FACE_KAPPA, kappa, trace[:PART])
    parts = jnp.concatenate(split_two(jnp.concatenate([value, kappa * trace[PART:]], 0)), 0)
    halo_out[1, 1] = shrink(dot(parts, send_hot[1]))
    images = Exchange(halo_out.at[1], halo_in.at[1], halo_send.at[1], halo_recv.at[1], 1)
    images.start(1)
    if len(rounds_of(group)) > 1:
        spread(1)
    image = result + lifted(terms, 0, 2)
    basis[1] = image
    stacked = stack(image)
    own, halves = faces_of(stacked, kappa, 0, 6)
    result, near, _ = inner(
        image, stacked, own, lambda face: folded(dot(halves[face ^ 1], local_hot[face]))
    )
    halo_out[1, 0] = shrink(dot(halves[0], send_hot[0]))
    images.start(0)
    value, flux = own[1]
    edge = 2.0 * outer(1) * down(face_weight * (value * (PENALTY * kappa * value - flux)))
    found = [across(down(field * field)), across(down(field * image)), across(down(image * image))]
    outside = outer(0) > 0.0
    kept[...] = near[0]
    _, (jump, mean, first, scaled) = coefficients(0, own[0], near[0])

    inside = jnp.where(outside, own[0][0], jump) * first + jnp.where(outside, own[0][1], mean) * scaled
    inside = jnp.where(neigh_ref[0:1, :] < cells, down(inside), 0.0)
    found.append(across(down(image * result) + edge + inside))
    lane = iota((1, ROWS), 1)
    message = jnp.zeros((1, ROWS), F32)
    for index, value in enumerate(found):
        message = jnp.where(lane == index, value, message)
    across_edge = dot_last(halves[0], ghost_hot[0])
    across_edge = across_edge[:FACE] + across_edge[FACE:]
    code = orient_ref[0:1, :]
    bit_rows = iota((8, cells), 0)
    bits = jnp.where(
        bit_rows == 0, lax.rem(code, 2), jnp.where(bit_rows == 1, jnp.where(code >= 2, 1, 0), 1)
    )
    bits = dot_last(bits.astype(F32).astype(BF), ghost_hot[0])
    slot_sign = (1.0 - first_odd * bits[0:1]) * (1.0 - second_odd * bits[1:2])
    slot_weight = face_weight * bits[2:3]
    slot_kappa = across_edge[FACE_KAPPA : FACE_KAPPA + 1]

    for index in range(1, len(rounds_of(group))):
        if index > 1:
            spread(index)
        if index < len(rounds_of(group)) - 1:
            gather(index)
    images.arrive(0)
    if len(rounds_of(group)) > 1:
        gather(len(rounds_of(group)) - 1)
    ghosts = widen(halo_in[1, 0])
    penalty = PENALTY * jnp.maximum(slot_kappa, ghosts[FACE_KAPPA : FACE_KAPPA + 1])
    jump = across_edge[:PART] - slot_sign * ghosts[:PART]
    mean = across_edge[PART:] - slot_sign * ghosts[PART:]
    shared = across(down(slot_weight * (jump * (penalty * jump - mean))))
    sums[me] = message + jnp.where(lane == 3, shared, 0.0)

    for_each_other(
        lambda device: pltpu.make_async_remote_copy(
            src_ref=sums.at[me],
            dst_ref=sums.at[me],
            send_sem=sum_send,
            recv_sem=sum_recv,
            device_id=device,
            device_id_type=MESH,
        ).start()
    )

    images.arrive(1)
    terms = []
    near[0] = kept[...]
    for face in range(2):
        terms += coefficients(face, own[face], with_ghosts(near[face], widen(halo_in[1, face]), face))[0]
    basis[2] = result + lifted(split_terms(terms), 0, 2)
    for copies in (moves, tags, halos, fars, images):
        copies.leave()
    rest = sums.at[pl.ds(1, ranks - 1)]
    pltpu.make_async_copy(rest, rest, sum_send).wait()
    pltpu.make_async_copy(rest, rest, sum_recv).wait()
    summed = jnp.sum(sums[...], 0)
    ratios = pltpu.roll(summed, ROWS - 1, 1) / summed
    low, mid, high = (ratios[:, index : index + 1] for index in range(3))
    scale = 1.0 / (low * mid * (high - mid))
    linear = mid * (high - low) * scale
    square = (mid - low) * scale
    linear_ref[...] = jnp.broadcast_to(linear, (1, cells))
    square_ref[...] = jnp.broadcast_to(square, (1, cells))


def body(shape, right_side, conductivity, destination, neighbour, orientation, send_list):
    cells = right_side.shape[1]
    ghost = send_list.shape[1]
    ranks = shape[0] * shape[1]
    forward, backward, columns = tables()
    vmem = pl.BlockSpec(memory_space=pltpu.VMEM)
    dma = pltpu.SemaphoreType.DMA
    operands = (
        right_side,
        conductivity[None],
        destination[None],
        neighbour,
        orientation,
        send_list,
        jnp.asarray(forward),
        jnp.asarray(backward),
        jnp.asarray(columns),
    )
    operands = tuple(pltpu.with_memory_space_constraint(item, pltpu.HBM) for item in operands)
    basis, linear, square = pl.pallas_call(
        functools.partial(kernel, shape),
        out_shape=(
            jax.ShapeDtypeStruct((3, ROWS, cells), F32),
            jax.ShapeDtypeStruct((1, cells), F32),
            jax.ShapeDtypeStruct((1, cells), F32),
        ),
        in_specs=[pl.BlockSpec(memory_space=pltpu.HBM)] * len(operands),
        out_specs=(vmem, vmem, vmem),
        scratch_shapes=[pltpu.VMEM(item.shape, item.dtype) for item in operands]
        + [
            pltpu.VMEM((ROWS, cells), F32),
            pltpu.VMEM((6, cells, cells), BF),
            pltpu.VMEM((2, ghost, cells), BF),
            pltpu.VMEM((2, cells, ghost), BF),
            pltpu.VMEM((2, MOVE, ROWS), F32),
            pltpu.VMEM((2, MOVE, ROWS), F32),
            pltpu.VMEM((2, MOVE // 2, ROWS), F32),
            pltpu.VMEM((2, MOVE // 2, ROWS), F32),
            pltpu.VMEM((2, 2, HALO, ghost), F32),
            pltpu.VMEM((2, 2, HALO, ghost), F32),
            pltpu.VMEM((ranks, 1, ROWS), F32),
            pltpu.VMEM((FACE, cells), F32),
            pltpu.VMEM((6, FACE, cells), F32),
            pltpu.VMEM((2, 1, ghost), F32),
            pltpu.VMEM((2, 1, ghost), F32),
            dma((2,)),
            dma((2,)),
            dma((len(operands),)),
            dma((2,)),
            dma((2,)),
            dma((2,)),
            dma((2,)),
            dma((2, 2)),
            dma((2, 2)),
            dma,
            dma,
            pltpu.SemaphoreType.REGULAR((len(rounds_of(shape[1])),)),
        ],
        compiler_params=pltpu.CompilerParams(
            collective_id=0, has_side_effects=True, vmem_limit_bytes=VMEM_LIMIT
        ),
    )(*operands)
    first, second, third = (basis[index, :BLOCK] for index in range(3))
    return linear * first - square * second, first - linear * second + square * third


def solution(mesh):
    both = ("curve", "group")
    shape = (mesh.shape["curve"], mesh.shape["group"])
    in_specs = (P(None, both), P(both), P(both), P(None, both), P(None, both), P(None, both))
    out_specs = (P(None, both), P(None, both))
    return jax.shard_map(
        functools.partial(body, shape),
        mesh=mesh,
        in_specs=in_specs,
        out_specs=out_specs,
        check_vma=False,
    )
```

```python
import functools

import jax
import jax.numpy as jnp
import numpy as np
from jax import lax
from jax.experimental import pallas as pl
from jax.experimental.pallas import tpu as pltpu
from jax.sharding import PartitionSpec as P

NODES = 5
BLOCK = 125
MOVE = 64
UNROLLED = 64
VMEM_LIMIT = 24 * 1024 * 1024
PENALTY = 80.0
MESH = pl.DeviceIdType.MESH
BF = jnp.bfloat16
F32 = jnp.float32

ROWS = 128
KAPPA = 125
TAG = 126
PART = 32
FACE = 2 * PART
FACE_KAPPA = 25
FACE_TAG = 26
HALO = PART + 24
FACE_LAST = 27

GAUSS_POINTS = (-0.906179845938664, -0.5384693101056831, 0.0, 0.5384693101056831, 0.906179845938664)
GAUSS_WEIGHTS = (
    0.2369268850561891,
    0.4786286704993665,
    0.5688888888888889,
    0.4786286704993665,
    0.2369268850561891,
)


def lagrange_value(points, position, location):
    out = 1.0
    for other in range(len(points)):
        if other != position:
            out = out * (location - points[other]) / (points[position] - points[other])
    return out


def lagrange_slope(points, position, location):
    total = 0.0
    for skipped in range(len(points)):
        if skipped == position:
            continue
        addend = 1.0 / (points[position] - points[skipped])
        for other in range(len(points)):
            if other != position and other != skipped:
                addend = addend * (location - points[other]) / (points[position] - points[other])
        total = total + addend
    return total


def along_axis(matrix, axis):
    five = np.eye(NODES)
    plane = np.eye(NODES * NODES)
    if axis == 0:
        return np.kron(matrix, plane)
    if axis == 1:
        return np.kron(five, np.kron(matrix, five))
    return np.kron(plane, matrix)


def split_table(table):
    high = table.astype(BF)
    low = (table - high.astype(np.float64)).astype(BF)
    return high, low


def tables():
    points = [0.5 * (value + 1.0) for value in GAUSS_POINTS]
    weights = np.array([0.5 * value for value in GAUSS_WEIGHTS])
    slopes = np.array([[lagrange_slope(points, p, points[q]) for p in range(NODES)] for q in range(NODES)])
    ends = [np.array([lagrange_value(points, p, at) for p in range(NODES)]) for at in (0.0, 1.0)]
    normals = [
        np.array([sign * lagrange_slope(points, p, at) for p in range(NODES)])
        for sign, at in ((-1.0, 0.0), (1.0, 1.0))
    ]
    cell_weight = np.kron(weights, np.kron(weights, weights))
    stiffness = np.zeros((BLOCK, BLOCK))
    for axis in range(3):
        grad = along_axis(slopes, axis)
        stiffness += grad.T @ (cell_weight[:, None] * grad)
    half = np.sqrt(0.5)
    parity_rows = np.zeros((NODES, NODES))
    for row, (a, b, sign) in enumerate(((0, 4, 1), (1, 3, 1), (2, 2, 1), (0, 4, -1), (1, 3, -1))):
        if a == b:
            parity_rows[row, a] = 1.0
        else:
            parity_rows[row, a] = half
            parity_rows[row, b] = sign * half
    parity = np.array([0, 0, 0, 1, 1])
    row_weight = weights[[0, 1, 2, 0, 1]]
    both = np.kron(parity_rows, parity_rows)
    count = NODES * NODES
    trace = np.zeros((6 * FACE, ROWS))
    for face in range(6):
        start = face * FACE
        trace[start : start + count, :BLOCK] = both @ along_axis(ends[face % 2][None, :], face // 2)
        trace[start + PART : start + PART + count, :BLOCK] = both @ along_axis(
            normals[face % 2][None, :], face // 2
        )
    lift = trace.T.copy()
    right = trace[FACE : 2 * FACE].copy()
    for face in range(6):
        trace[face * FACE + FACE_KAPPA, KAPPA] = 1.0
    first = np.zeros((6 * FACE + 2 * ROWS, ROWS))
    first[: 6 * FACE] = trace
    first[6 * FACE : 6 * FACE + BLOCK, :BLOCK] = stiffness
    first[6 * FACE + ROWS : 7 * FACE + ROWS, :BLOCK] = right[:, :BLOCK] @ stiffness
    first[7 * FACE + ROWS :, :BLOCK] = right[:, :BLOCK] * cell_weight
    high, low = split_table(first)
    forward = np.concatenate([high, high, low], 1)
    backward = np.concatenate(split_table(lift) + split_table(right @ lift), 0)
    columns = np.zeros((ROWS, ROWS), np.float32)
    columns[:BLOCK, 0] = cell_weight
    columns[:count, 1] = np.kron(row_weight, row_weight)
    columns[:count, 2] = 2.0 * np.kron(parity, np.ones(NODES))
    columns[:count, 3] = 2.0 * np.kron(np.ones(NODES), parity)
    return forward, backward, columns


def split_two(value):
    high = value.astype(BF)
    low = (value - high.astype(F32)).astype(BF)
    return high, low


def split_three(value):
    high = value.astype(BF)
    rest = value - high.astype(F32)
    mid = rest.astype(BF)
    return high, mid, (rest - mid.astype(F32)).astype(BF)


def one_hot(left, right):
    return jnp.where(left == right, 1.0, 0.0).astype(BF)


def dot(left, right):
    return jnp.dot(left, right, preferred_element_type=F32)


def dot_last(left, right):
    return lax.dot_general(left, right, (((1,), (1,)), ((), ())), preferred_element_type=F32)


def iota(shape, dim):
    return lax.broadcasted_iota(jnp.int32, shape, dim)


def rounds_of(group):
    rounds, reach = [(1, 2)], 2
    while reach < group - 1:
        rounds.append((reach,))
        reach *= 2
    return rounds


def kernel(
    shape,
    rhs_hbm,
    cond_hbm,
    dest_hbm,
    neigh_hbm,
    orient_hbm,
    list_hbm,
    forward_hbm,
    backward_hbm,
    column_hbm,
    basis,
    linear_ref,
    square_ref,
    rhs_ref,
    cond_ref,
    dest_ref,
    neigh_ref,
    orient_ref,
    list_ref,
    forward_ref,
    backward_ref,
    column_ref,
    payload,
    local_hot,
    ghost_hot,
    send_hot,
    packed,
    moved,
    far_out,
    far_in,
    halo_out,
    halo_in,
    sums,
    kept,
    shared,
    slot_out,
    slot_in,
    edge_in,
    edge_send,
    edge_recv,
    near_ref,
    tag_out,
    tag_in,
    tag_send,
    tag_recv,
    load_sem,
    move_send,
    move_recv,
    far_send,
    far_recv,
    halo_send,
    halo_recv,
    sum_send,
    sum_recv,
    seen,
):
    curve, group = shape
    ranks = curve * group
    cells = rhs_ref.shape[1]
    ghost = list_ref.shape[1]
    me = lax.axis_index("curve") * group + lax.axis_index("group")

    def place(rank):
        return (rank // group, lax.rem(rank, group))

    def other(step):
        return place(lax.rem(me + step, ranks))

    class Exchange:
        def __init__(self, source, target, send_sem, recv_sem, reach):
            self.there = (me >= reach, me + reach < ranks)
            self.copies = [
                pltpu.make_async_remote_copy(
                    src_ref=source.at[side],
                    dst_ref=target.at[1 - side],
                    send_sem=send_sem.at[side],
                    recv_sem=recv_sem.at[1 - side],
                    device_id=device,
                    device_id_type=MESH,
                )
                for side, device in ((0, other(ranks - reach)), (1, other(reach)))
            ]

        def start(self, side):
            pl.when(self.there[side])(self.copies[side].start)

        def arrive(self, side):
            pl.when(self.there[side])(self.copies[1 - side].wait_recv)

        def leave(self):
            for side in range(2):
                pl.when(self.there[side])(self.copies[side].wait_send)

    def clear(reach, refs):
        for side, missing in ((0, me < reach), (1, me + reach >= ranks)):

            @pl.when(missing)
            def _():
                for ref in refs:
                    ref[side] = jnp.zeros(ref.shape[1:], ref.dtype)

    barrier = pltpu.get_barrier_semaphore()

    my_curve, my_group = lax.axis_index("curve"), lax.axis_index("group")

    def for_each_other(act):
        def one(to_group):
            for step in range(curve):
                to = (lax.rem(my_curve + step, curve), to_group)
                if step:
                    act(to)
                else:
                    pl.when(to_group != my_group)(functools.partial(act, to))

        if ranks <= UNROLLED:
            for to_group in range(group):
                one(to_group)
        else:
            pl.loop(0, group)(one)

    def signal(semaphore, device):
        pl.semaphore_signal(semaphore, inc=1, device_id=device, device_id_type=MESH)

    wide_group = group > 2
    odd = lax.rem(my_curve, 2) == 1
    paired = odd & (my_curve + 1 < curve) & wide_group
    helps = paired & (my_group == 0)
    reports = paired & (my_group == group - 1)
    defers = jnp.logical_not(odd) & (my_curve > 0) & (my_group == 0) & wide_group
    greeted = curve - 1 + helps.astype(jnp.int32) + reports.astype(jnp.int32)
    pl.when(reports)(functools.partial(signal, barrier, (my_curve, 0)))
    pl.when(helps)(functools.partial(signal, barrier, (my_curve, group - 1)))
    for step in (2, 1):
        for there, device in (
            (me + step < ranks, other(step)),
            (me >= step, other(ranks - step)),
        ):
            pl.when(there)(functools.partial(signal, barrier, device))
            greeted = greeted + there.astype(jnp.int32)
    for step in range(1, curve):
        signal(barrier, (lax.rem(my_curve + step, curve), my_group))

    def spread(index):
        for step in rounds_of(group)[index]:
            for there, to in (
                (my_group + step < group, my_group + step),
                (my_group >= step, my_group - step),
            ):
                pl.when(there)(functools.partial(signal, seen.at[index], (my_curve, to)))

    def gather(index):
        count = 0
        for step in rounds_of(group)[index]:
            count = count + (my_group + step < group).astype(jnp.int32)
            count = count + (my_group >= step).astype(jnp.int32)
        pl.semaphore_wait(seen.at[index], count)

    loads = [
        pltpu.make_async_copy(source, target, load_sem.at[index])
        for index, (source, target) in enumerate(
            (
                (dest_hbm, dest_ref),
                (list_hbm, list_ref),
                (cond_hbm, cond_ref),
                (rhs_hbm, rhs_ref),
                (forward_hbm, forward_ref),
                (neigh_hbm, neigh_ref),
                (orient_hbm, orient_ref),
                (column_hbm, column_ref),
                (backward_hbm, backward_ref),
            )
        )
    ]
    for load in loads:
        load.start()
    clear(1, (moved, tag_in, halo_in.at[0], halo_in.at[1]))
    clear(2, (far_in,))
    for load in loads[:4]:
        load.wait()

    def faces_of(stacked, kappa, first, last):
        part = dot(forward_ref[first * FACE : last * FACE, :], stacked)
        own, halves = [], []
        for index in range(last - first):
            value = part[index * FACE : index * FACE + PART]
            flux = kappa * part[index * FACE + PART : (index + 1) * FACE]
            own.append((value, flux))
            halves.append(jnp.concatenate(split_two(jnp.concatenate([value, flux], 0)), 0))
        return own, halves

    offset = dest_ref[...] - me * cells
    goes_left = offset < 0
    goes_right = offset >= cells
    slot = jnp.where(goes_left, offset + cells, jnp.where(goes_right, offset - cells, offset))
    payload[0:BLOCK, :] = rhs_ref[...]
    payload[KAPPA : KAPPA + 1, :] = cond_ref[...]
    payload[TAG : TAG + 1, :] = (slot + 1).astype(F32)
    payload[TAG + 1 : TAG + 2, :] = jnp.zeros((1, cells), F32)
    high, mid, low = split_three(payload[...])
    parts = jnp.concatenate([high, mid, low], 0)
    row8 = iota((8, cells), 0)
    leaving = jnp.where(
        row8 == 0,
        jnp.where(goes_left, 1.0, 0.0),
        jnp.where(row8 == 1, jnp.where(goes_right, 1.0, 0.0), 0.0),
    ).astype(BF)
    triangle = jnp.where(iota((cells, cells), 0) <= iota((cells, cells), 1), 1.0, 0.0).astype(BF)
    order = dot(leaving, triangle).astype(jnp.int32) - 1
    slots = iota((MOVE, cells), 0)
    pick = jnp.concatenate(
        [
            one_hot(jnp.where(goes_left, order[0:1], -1), slots),
            one_hot(jnp.where(goes_right, order[1:2], -1), slots),
        ],
        0,
    )
    chosen = dot_last(pick, parts)
    chosen = chosen[:, :ROWS] + chosen[:, ROWS : 2 * ROWS] + chosen[:, 2 * ROWS :]
    packed[0] = chosen[:MOVE]
    packed[1] = chosen[MOVE:]

    lists = list_ref[...].astype(F32)
    for side in range(2):
        tag_out[side] = lists[side : side + 1, :]

    pl.semaphore_wait(barrier, greeted)

    moves = Exchange(packed, moved, move_send, move_recv, 1)
    tags = Exchange(tag_out, tag_in, tag_send, tag_recv, 1)
    moves.start(0)
    pl.when(my_group > 0)(functools.partial(moves.start, 1))
    for side in range(2):
        tags.start(side)

    for load in loads[4:]:
        load.wait()

    old_halves = faces_of(jnp.concatenate([high, mid, high], 0), cond_ref[...], 0, 2)[1]
    offset_column = jnp.broadcast_to(offset.astype(F32), (8, cells)).T[:, 0:1]
    halo_rows = iota((HALO, ghost), 0)

    def shrink(out):
        out = out[:FACE] + out[FACE:]
        return jnp.where(halo_rows == FACE_LAST, out[HALO : HALO + 1], out[:HALO])

    def widen(message):
        last = message[FACE_LAST : FACE_LAST + 1]
        rest = jnp.where(iota((FACE - HALO, ghost), 0) == 0, last, 0.0)
        return jnp.concatenate([message, rest], 0)

    for side in range(2):
        hot = one_hot(offset_column, lists[side : side + 1, :])
        out = dot(old_halves[side], hot)
        halo_out[0, side] = shrink(out)
    lanes = iota((2 * MOVE, ROWS), 1)
    tagged = jnp.where(lanes == FACE_TAG, chosen[:, TAG : TAG + 1], 0.0)
    leaving_low = dot_last(pick, old_halves[0]) + tagged
    leaving_high = dot_last(pick, old_halves[1]) + tagged
    leaving_low = leaving_low[:, :FACE] + leaving_low[:, FACE:]
    leaving_high = leaving_high[:, :FACE] + leaving_high[:, FACE:]
    middle = MOVE // 2
    far_out[0] = jnp.concatenate([leaving_low[:middle], leaving_low[middle:MOVE]], 1)
    far_out[1] = jnp.concatenate([leaving_high[MOVE : MOVE + middle], leaving_high[MOVE + middle :]], 1)

    halos = Exchange(halo_out.at[0], halo_in.at[0], halo_send.at[0], halo_recv.at[0], 1)
    fars = Exchange(far_out, far_in, far_send, far_recv, 2)
    halos.start(0)
    pl.when(my_group == 0)(functools.partial(moves.start, 1))
    for side in range(2):
        fars.start(side)
    halos.start(1)
    spread(0)

    stay = one_hot(iota((cells, cells), 0), offset)
    arrived = dot_last(parts, stay)
    cell_rows = iota((cells, cells), 0)
    ghost_rows = iota((ghost, cells), 0)
    for face in range(6):
        local_hot[face] = one_hot(neigh_ref[face : face + 1, :], cell_rows)
    for side in range(2):
        ghost_hot[side] = one_hot(
            neigh_ref[side : side + 1, :] - (cells + side * ghost), ghost_rows
        )
        send_hot[side] = one_hot(list_ref[side : side + 1, :], iota((cells, ghost), 0))

    def folded(value):
        half = value.shape[0] // 2
        return value[:half] + value[half:]

    arrived = arrived[:ROWS] + arrived[ROWS : 2 * ROWS] + arrived[2 * ROWS :]
    high, low = split_two(arrived)
    stay_halves = faces_of(
        jnp.concatenate([high, low, high], 0), arrived[KAPPA : KAPPA + 1], 0, 6
    )[1]
    for face in range(6):
        near_ref[face] = folded(dot(stay_halves[face ^ 1], local_hot[face]))
    payload[...] = arrived

    for side in range(2):
        moves.arrive(side)
        tags.arrive(side)
    record = moved[...].reshape(2 * MOVE, ROWS)
    landing = record[:, TAG : TAG + 1].astype(jnp.int32) - 1
    record = record.T
    high, mid, low = split_three(record)
    placed = dot(
        jnp.concatenate([high, mid, low], 0), one_hot(landing, iota((2 * MOVE, cells), 1))
    )
    arrived = payload[...] + (placed[:ROWS] + placed[ROWS : 2 * ROWS] + placed[2 * ROWS :])
    moved_halves = faces_of(
        jnp.concatenate([high, mid, high], 0), record[KAPPA : KAPPA + 1], 0, 6
    )[1]
    landing = jnp.where(landing < 0, -2, landing)

    def near_old(face):
        hot = one_hot(landing, neigh_ref[face : face + 1, :])
        return near_ref[face] + folded(dot(moved_halves[face ^ 1], hot))

    rows = iota((ROWS, cells), 0)
    field = jnp.where(rows < BLOCK, arrived, 0.0)
    kappa = arrived[KAPPA : KAPPA + 1]
    cell_weight = column_ref[:, 0:1]
    face_weight = column_ref[0:PART, 1:2]
    first_odd = column_ref[0:PART, 2:3]
    second_odd = column_ref[0:PART, 3:4]

    def signs(face):
        code = orient_ref[face : face + 1, :]
        first_bit = jnp.where(lax.rem(code, 2) == 1, 1.0, 0.0)
        second_bit = jnp.where(code >= 2, 1.0, 0.0)
        return (1.0 - first_odd * first_bit) * (1.0 - second_odd * second_bit)

    def outer(face):
        return jnp.where(neigh_ref[face : face + 1, :] < 0, 1.0, 0.0)

    def coefficients(face, own, near):
        value, flux = own
        sign = signs(face)
        outside = outer(face)
        near_kappa = near[FACE_KAPPA : FACE_KAPPA + 1] + outside * kappa
        penalty = PENALTY * jnp.maximum(kappa, near_kappa)
        jump = value - (sign * near[:PART] - outside * value)
        mean = flux - (sign * near[PART:] - outside * flux)
        scaled = -0.5 * (face_weight * jump)
        first = face_weight * (penalty * jump - 0.5 * mean)
        return (first, kappa * scaled), (jump, mean, first, scaled)

    def lifted(parts, first, last):
        high, low = parts
        both = dot(backward_ref[0 : 2 * ROWS, first * FACE : last * FACE], high)
        rest = dot(backward_ref[0:ROWS, first * FACE : last * FACE], low)
        return both[:ROWS] + both[ROWS:] + rest

    def traced(parts, first, last):
        high, low = parts
        both = dot(backward_ref[2 * ROWS :, first * FACE : last * FACE], high)
        rest = dot(backward_ref[2 * ROWS : 2 * ROWS + FACE, first * FACE : last * FACE], low)
        return both[:FACE] + both[FACE:] + rest

    def split_terms(terms):
        return split_two(jnp.concatenate(terms, 0))

    def stack(field):
        high, low = split_two(jnp.where(rows == KAPPA, kappa, field))
        return jnp.concatenate([high, low, high], 0)

    def inner(field, stacked, own, near):
        terms = []
        for face in range(2, 6):
            terms += coefficients(face, own[face], near(face))[0]
        stiff = dot(forward_ref[6 * FACE : 6 * FACE + ROWS, :], stacked)
        terms = split_terms(terms)
        result = lifted(terms, 2, 6) + cell_weight * field + kappa * stiff
        return result, [near(face) for face in range(2)], terms

    def with_ghosts(near, ghosts, side):
        return near + folded(dot(jnp.concatenate(split_two(ghosts), 0), ghost_hot[side]))

    def down(value):
        return jnp.sum(value, 0, keepdims=True)

    def across(value):
        return jnp.sum(value, 1, keepdims=True)

    basis[0] = field
    stacked = stack(field)
    own = faces_of(stacked, kappa, 0, 6)[0]
    result, near, terms = inner(field, stacked, own, near_old)
    volume = dot(forward_ref[6 * FACE + ROWS :, :], stacked)
    trace = traced(terms, 2, 6) + kappa * volume[:FACE] + volume[FACE:]
    marks = []
    for side in range(2):
        mark = jnp.concatenate(split_two(jnp.broadcast_to(tag_in[side] + 1.0, (8, ghost))), 0)
        mark = dot(mark, ghost_hot[side])
        mark = mark[0:1] + mark[8:9]
        marks.append(jnp.where(mark == 0.0, -1.0, mark))
    for side in range(2):
        halos.arrive(side)
        fars.arrive(side)
    gather(0)
    terms = []
    for face in range(2):
        gone = leaving_high[:MOVE] if face == 0 else leaving_low[MOVE:]
        far = far_in[face]
        wide = jnp.concatenate([far[:, :FACE], far[:, FACE:], gone], 0)
        hot = one_hot(wide[:, FACE_TAG : FACE_TAG + 1], marks[face])
        placed = dot(jnp.concatenate(split_two(wide.T), 0), hot)
        ghosts = with_ghosts(near[face], widen(halo_in[0, face]), face) + folded(placed)
        terms += coefficients(face, own[face], ghosts)[0]
    terms = split_terms(terms)
    trace = trace + traced(terms, 0, 2)
    value = jnp.where(iota((PART, cells), 0) == FACE_KAPPA, kappa, trace[:PART])
    parts = jnp.concatenate(split_two(jnp.concatenate([value, kappa * trace[PART:]], 0)), 0)
    halo_out[1, 1] = shrink(dot(parts, send_hot[1]))
    images = Exchange(halo_out.at[1], halo_in.at[1], halo_send.at[1], halo_recv.at[1], 1)
    report = pltpu.make_async_remote_copy(
        src_ref=halo_out.at[1, 1],
        dst_ref=edge_in,
        send_sem=edge_send.at[0],
        recv_sem=edge_recv.at[0],
        device_id=(my_curve, 0),
        device_id_type=MESH,
    )
    pl.when(reports)(report.start)
    images.start(1)
    if len(rounds_of(group)) > 1:
        spread(1)
    image = result + lifted(terms, 0, 2)
    basis[1] = image
    stacked = stack(image)
    own, halves = faces_of(stacked, kappa, 0, 6)
    result, near, _ = inner(
        image, stacked, own, lambda face: folded(dot(halves[face ^ 1], local_hot[face]))
    )
    halo_out[1, 0] = shrink(dot(halves[0], send_hot[0]))
    images.start(0)
    value, flux = own[1]
    edge = 2.0 * outer(1) * down(face_weight * (value * (PENALTY * kappa * value - flux)))
    found = [across(down(field * field)), across(down(field * image)), across(down(image * image))]
    outside = outer(0) > 0.0
    kept[...] = near[0]
    _, (jump, mean, first, scaled) = coefficients(0, own[0], near[0])

    inside = jnp.where(outside, own[0][0], jump) * first + jnp.where(outside, own[0][1], mean) * scaled
    inside = jnp.where(neigh_ref[0:1, :] < cells, down(inside), 0.0)
    found.append(across(down(image * result) + edge + inside))
    lane = iota((1, ROWS), 1)
    message = jnp.zeros((1, ROWS), F32)
    for index, value in enumerate(found):
        message = jnp.where(lax.rem(lane, 4) == index, value, message)
    across_edge = dot_last(halves[0], ghost_hot[0])
    across_edge = across_edge[:FACE] + across_edge[FACE:]
    code = orient_ref[0:1, :]
    bit_rows = iota((8, cells), 0)
    bits = jnp.where(
        bit_rows == 0, lax.rem(code, 2), jnp.where(bit_rows == 1, jnp.where(code >= 2, 1, 0), 1)
    )
    bits = dot_last(bits.astype(F32).astype(BF), ghost_hot[0])
    for index in range(3):
        row = iota((FACE, ghost), 0) == FACE_TAG + index
        across_edge = jnp.where(row, bits[index : index + 1], across_edge)
    slot_out[...] = across_edge
    defer = pltpu.make_async_remote_copy(
        src_ref=slot_out,
        dst_ref=slot_in,
        send_sem=edge_send.at[1],
        recv_sem=edge_recv.at[1],
        device_id=(lax.rem(my_curve + curve - 1, curve), my_group),
        device_id_type=MESH,
    )
    pl.when(defers)(defer.start)

    def edge_energy(mine, ghosts):
        bit = mine[FACE_TAG : FACE_TAG + 3]
        sign = (1.0 - first_odd * bit[0:1]) * (1.0 - second_odd * bit[1:2])
        kappas = jnp.maximum(mine[FACE_KAPPA : FACE_KAPPA + 1], ghosts[FACE_KAPPA : FACE_KAPPA + 1])
        jump = mine[:PART] - sign * ghosts[:PART]
        mean = mine[PART:] - sign * ghosts[PART:]
        energy = face_weight * bit[2:3] * (jump * (PENALTY * kappas * jump - mean))
        return jnp.broadcast_to(across(down(energy)), (1, ROWS))

    for index in range(1, len(rounds_of(group))):
        if index > 1:
            spread(index)
        if index < len(rounds_of(group)) - 1:
            gather(index)
    shared[...] = jnp.zeros((1, ROWS), F32)

    @pl.when(jnp.logical_not(defers))
    def _():
        images.arrive(0)
        shared[...] = edge_energy(slot_out[...], widen(halo_in[1, 0]))

    if len(rounds_of(group)) > 1:
        gather(len(rounds_of(group)) - 1)

    @pl.when(helps)
    def _():
        defer.wait_recv()
        report.wait_recv()
        shared[...] += edge_energy(slot_in[...], widen(edge_in[...]))

    sums[me] = message + jnp.where(lax.rem(lane, 4) == 3, shared[...], 0.0)

    for_each_other(
        lambda device: pltpu.make_async_remote_copy(
            src_ref=sums.at[me],
            dst_ref=sums.at[me],
            send_sem=sum_send,
            recv_sem=sum_recv,
            device_id=device,
            device_id_type=MESH,
        ).start()
    )

    pl.when(defers)(functools.partial(images.arrive, 0))
    images.arrive(1)
    pl.when(defers)(defer.wait_send)
    pl.when(reports)(report.wait_send)
    terms = []
    near[0] = kept[...]
    for face in range(2):
        terms += coefficients(face, own[face], with_ghosts(near[face], widen(halo_in[1, face]), face))[0]
    basis[2] = result + lifted(split_terms(terms), 0, 2)
    for copies in (moves, tags, halos, fars, images):
        copies.leave()
    rest = sums.at[pl.ds(1, ranks - 1)]
    pltpu.make_async_copy(rest, rest, sum_send).wait()
    pltpu.make_async_copy(rest, rest, sum_recv).wait()
    summed = jnp.sum(sums[...], 0)
    turns = [summed] + [pltpu.roll(summed, turn, 1) for turn in range(1, 4)]
    phase = lax.rem(lane, 4)
    totals = []
    for index in range(4):
        total = turns[3]
        for turn in range(3):
            total = jnp.where(lax.rem(phase + 4 - turn, 4) == index, turns[turn], total)
        totals.append(total)
    low, mid, high = (totals[index + 1] / totals[index] for index in range(3))
    scale = 1.0 / (low * mid * (high - mid))
    linear = mid * (high - low) * scale
    square = (mid - low) * scale
    linear_ref[...] = jnp.concatenate([linear] * (cells // ROWS), 1)
    square_ref[...] = jnp.concatenate([square] * (cells // ROWS), 1)


def body(shape, right_side, conductivity, destination, neighbour, orientation, send_list):
    cells = right_side.shape[1]
    ghost = send_list.shape[1]
    ranks = shape[0] * shape[1]
    forward, backward, columns = tables()
    vmem = pl.BlockSpec(memory_space=pltpu.VMEM)
    dma = pltpu.SemaphoreType.DMA
    operands = (
        right_side,
        conductivity[None],
        destination[None],
        neighbour,
        orientation,
        send_list,
        jnp.asarray(forward),
        jnp.asarray(backward),
        jnp.asarray(columns),
    )
    operands = tuple(pltpu.with_memory_space_constraint(item, pltpu.HBM) for item in operands)
    basis, linear, square = pl.pallas_call(
        functools.partial(kernel, shape),
        out_shape=(
            jax.ShapeDtypeStruct((3, ROWS, cells), F32),
            jax.ShapeDtypeStruct((1, cells), F32),
            jax.ShapeDtypeStruct((1, cells), F32),
        ),
        in_specs=[pl.BlockSpec(memory_space=pltpu.HBM)] * len(operands),
        out_specs=(vmem, vmem, vmem),
        scratch_shapes=[pltpu.VMEM(item.shape, item.dtype) for item in operands]
        + [
            pltpu.VMEM((ROWS, cells), F32),
            pltpu.VMEM((6, cells, cells), BF),
            pltpu.VMEM((2, ghost, cells), BF),
            pltpu.VMEM((2, cells, ghost), BF),
            pltpu.VMEM((2, MOVE, ROWS), F32),
            pltpu.VMEM((2, MOVE, ROWS), F32),
            pltpu.VMEM((2, MOVE // 2, ROWS), F32),
            pltpu.VMEM((2, MOVE // 2, ROWS), F32),
            pltpu.VMEM((2, 2, HALO, ghost), F32),
            pltpu.VMEM((2, 2, HALO, ghost), F32),
            pltpu.VMEM((ranks, 1, ROWS), F32),
            pltpu.VMEM((FACE, cells), F32),
            pltpu.VMEM((1, ROWS), F32),
            pltpu.VMEM((FACE, ghost), F32),
            pltpu.VMEM((FACE, ghost), F32),
            pltpu.VMEM((HALO, ghost), F32),
            dma((2,)),
            dma((2,)),
            pltpu.VMEM((6, FACE, cells), F32),
            pltpu.VMEM((2, 1, ghost), F32),
            pltpu.VMEM((2, 1, ghost), F32),
            dma((2,)),
            dma((2,)),
            dma((len(operands),)),
            dma((2,)),
            dma((2,)),
            dma((2,)),
            dma((2,)),
            dma((2, 2)),
            dma((2, 2)),
            dma,
            dma,
            pltpu.SemaphoreType.REGULAR((len(rounds_of(shape[1])),)),
        ],
        compiler_params=pltpu.CompilerParams(
            collective_id=0, has_side_effects=True, vmem_limit_bytes=VMEM_LIMIT
        ),
    )(*operands)
    first, second, third = (basis[index, :BLOCK] for index in range(3))
    return linear * first - square * second, first - linear * second + square * third


def solution(mesh):
    both = ("curve", "group")
    shape = (mesh.shape["curve"], mesh.shape["group"])
    in_specs = (P(None, both), P(both), P(both), P(None, both), P(None, both), P(None, both))
    out_specs = (P(None, both), P(None, both))
    return jax.shard_map(
        functools.partial(body, shape),
        mesh=mesh,
        in_specs=in_specs,
        out_specs=out_specs,
        check_vma=False,
    )
```

```python
import functools

import jax
import jax.numpy as jnp
import numpy as np
from jax import lax
from jax.experimental import pallas as pl
from jax.experimental.pallas import tpu as pltpu
from jax.sharding import PartitionSpec as P

NODES = 5
BLOCK = 125
MOVE = 64
UNROLLED = 64
VMEM_LIMIT = 24 * 1024 * 1024
PENALTY = 80.0
MESH = pl.DeviceIdType.MESH
BF = jnp.bfloat16
F32 = jnp.float32

ROWS = 128
KAPPA = 125
TAG = 126
PART = 32
FACE = 2 * PART
FACE_KAPPA = 25
FACE_TAG = 26
HALO = PART + 24
FACE_LAST = 27

GAUSS_POINTS = (-0.906179845938664, -0.5384693101056831, 0.0, 0.5384693101056831, 0.906179845938664)
GAUSS_WEIGHTS = (
    0.2369268850561891,
    0.4786286704993665,
    0.5688888888888889,
    0.4786286704993665,
    0.2369268850561891,
)


def lagrange_value(points, position, location):
    out = 1.0
    for other in range(len(points)):
        if other != position:
            out = out * (location - points[other]) / (points[position] - points[other])
    return out


def lagrange_slope(points, position, location):
    total = 0.0
    for skipped in range(len(points)):
        if skipped == position:
            continue
        addend = 1.0 / (points[position] - points[skipped])
        for other in range(len(points)):
            if other != position and other != skipped:
                addend = addend * (location - points[other]) / (points[position] - points[other])
        total = total + addend
    return total


def along_axis(matrix, axis):
    five = np.eye(NODES)
    plane = np.eye(NODES * NODES)
    if axis == 0:
        return np.kron(matrix, plane)
    if axis == 1:
        return np.kron(five, np.kron(matrix, five))
    return np.kron(plane, matrix)


def split_table(table):
    high = table.astype(BF)
    low = (table - high.astype(np.float64)).astype(BF)
    return high, low


def tables():
    points = [0.5 * (value + 1.0) for value in GAUSS_POINTS]
    weights = np.array([0.5 * value for value in GAUSS_WEIGHTS])
    slopes = np.array([[lagrange_slope(points, p, points[q]) for p in range(NODES)] for q in range(NODES)])
    ends = [np.array([lagrange_value(points, p, at) for p in range(NODES)]) for at in (0.0, 1.0)]
    normals = [
        np.array([sign * lagrange_slope(points, p, at) for p in range(NODES)])
        for sign, at in ((-1.0, 0.0), (1.0, 1.0))
    ]
    cell_weight = np.kron(weights, np.kron(weights, weights))
    stiffness = np.zeros((BLOCK, BLOCK))
    for axis in range(3):
        grad = along_axis(slopes, axis)
        stiffness += grad.T @ (cell_weight[:, None] * grad)
    half = np.sqrt(0.5)
    parity_rows = np.zeros((NODES, NODES))
    for row, (a, b, sign) in enumerate(((0, 4, 1), (1, 3, 1), (2, 2, 1), (0, 4, -1), (1, 3, -1))):
        if a == b:
            parity_rows[row, a] = 1.0
        else:
            parity_rows[row, a] = half
            parity_rows[row, b] = sign * half
    parity = np.array([0, 0, 0, 1, 1])
    row_weight = weights[[0, 1, 2, 0, 1]]
    both = np.kron(parity_rows, parity_rows)
    count = NODES * NODES
    trace = np.zeros((6 * FACE, ROWS))
    for face in range(6):
        start = face * FACE
        trace[start : start + count, :BLOCK] = both @ along_axis(ends[face % 2][None, :], face // 2)
        trace[start + PART : start + PART + count, :BLOCK] = both @ along_axis(
            normals[face % 2][None, :], face // 2
        )
    lift = trace.T.copy()
    right = trace[FACE : 2 * FACE].copy()
    for face in range(6):
        trace[face * FACE + FACE_KAPPA, KAPPA] = 1.0
    first = np.zeros((6 * FACE + 2 * ROWS, ROWS))
    first[: 6 * FACE] = trace
    first[6 * FACE : 6 * FACE + BLOCK, :BLOCK] = stiffness
    first[6 * FACE + ROWS : 7 * FACE + ROWS, :BLOCK] = right[:, :BLOCK] @ stiffness
    first[7 * FACE + ROWS :, :BLOCK] = right[:, :BLOCK] * cell_weight
    high, low = split_table(first)
    forward = np.concatenate([high, high, low], 1)
    backward = np.concatenate(split_table(lift) + split_table(right @ lift), 0)
    columns = np.zeros((ROWS, ROWS), np.float32)
    columns[:BLOCK, 0] = cell_weight
    columns[:count, 1] = np.kron(row_weight, row_weight)
    columns[:count, 2] = 2.0 * np.kron(parity, np.ones(NODES))
    columns[:count, 3] = 2.0 * np.kron(np.ones(NODES), parity)
    return forward, backward, columns


def split_two(value):
    high = value.astype(BF)
    low = (value - high.astype(F32)).astype(BF)
    return high, low


def split_three(value):
    high = value.astype(BF)
    rest = value - high.astype(F32)
    mid = rest.astype(BF)
    return high, mid, (rest - mid.astype(F32)).astype(BF)


def one_hot(left, right):
    return jnp.where(left == right, 1.0, 0.0).astype(BF)


def dot(left, right):
    return jnp.dot(left, right, preferred_element_type=F32)


def dot_last(left, right):
    return lax.dot_general(left, right, (((1,), (1,)), ((), ())), preferred_element_type=F32)


def iota(shape, dim):
    return lax.broadcasted_iota(jnp.int32, shape, dim)


def rounds_of(group):
    rounds, reach = [(1, 2)], 2
    while reach < group - 1:
        rounds.append((reach,))
        reach *= 2
    return rounds


def kernel(
    shape,
    rhs_hbm,
    cond_hbm,
    dest_hbm,
    neigh_hbm,
    orient_hbm,
    list_hbm,
    forward_hbm,
    backward_hbm,
    column_hbm,
    basis,
    linear_ref,
    square_ref,
    rhs_ref,
    cond_ref,
    dest_ref,
    neigh_ref,
    orient_ref,
    list_ref,
    forward_ref,
    backward_ref,
    column_ref,
    payload,
    local_hot,
    ghost_hot,
    send_hot,
    packed,
    moved,
    far_out,
    far_in,
    halo_out,
    halo_in,
    sums,
    kept,
    shared,
    slot_out,
    slot_in,
    edge_in,
    edge_send,
    edge_recv,
    near_ref,
    tag_out,
    tag_in,
    tag_send,
    tag_recv,
    load_sem,
    move_send,
    move_recv,
    far_send,
    far_recv,
    halo_send,
    halo_recv,
    sum_send,
    sum_recv,
    seen,
):
    curve, group = shape
    ranks = curve * group
    cells = rhs_ref.shape[1]
    ghost = list_ref.shape[1]
    me = lax.axis_index("curve") * group + lax.axis_index("group")

    def place(rank):
        return (rank // group, lax.rem(rank, group))

    def other(step):
        return place(lax.rem(me + step, ranks))

    class Exchange:
        def __init__(self, source, target, send_sem, recv_sem, reach):
            self.there = (me >= reach, me + reach < ranks)
            self.copies = [
                pltpu.make_async_remote_copy(
                    src_ref=source.at[side],
                    dst_ref=target.at[1 - side],
                    send_sem=send_sem.at[side],
                    recv_sem=recv_sem.at[1 - side],
                    device_id=device,
                    device_id_type=MESH,
                )
                for side, device in ((0, other(ranks - reach)), (1, other(reach)))
            ]

        def start(self, side):
            pl.when(self.there[side])(self.copies[side].start)

        def arrive(self, side):
            pl.when(self.there[side])(self.copies[1 - side].wait_recv)

        def leave(self):
            for side in range(2):
                pl.when(self.there[side])(self.copies[side].wait_send)

    def clear(reach, refs):
        for side, missing in ((0, me < reach), (1, me + reach >= ranks)):

            @pl.when(missing)
            def _():
                for ref in refs:
                    ref[side] = jnp.zeros(ref.shape[1:], ref.dtype)

    barrier = pltpu.get_barrier_semaphore()

    my_curve, my_group = lax.axis_index("curve"), lax.axis_index("group")

    def for_each_other(act):
        def one(to_group):
            for step in range(curve):
                to = (lax.rem(my_curve + step, curve), to_group)
                if step:
                    act(to)
                else:
                    pl.when(to_group != my_group)(functools.partial(act, to))

        if ranks <= UNROLLED:
            for to_group in range(group):
                one(to_group)
        else:
            pl.loop(0, group)(one)

    def signal(semaphore, device):
        pl.semaphore_signal(semaphore, inc=1, device_id=device, device_id_type=MESH)

    wide_group = group > 2
    odd = lax.rem(my_curve, 2) == 1
    paired = odd & (my_curve + 1 < curve) & wide_group
    helps = paired & (my_group == 0)
    reports = paired & (my_group == group - 1)
    defers = jnp.logical_not(odd) & (my_curve > 0) & (my_group == 0) & wide_group
    greeted = curve - 1 + helps.astype(jnp.int32) + reports.astype(jnp.int32)
    pl.when(reports)(functools.partial(signal, barrier, (my_curve, 0)))
    pl.when(helps)(functools.partial(signal, barrier, (my_curve, group - 1)))
    for step in (2, 1):
        for there, device in (
            (me + step < ranks, other(step)),
            (me >= step, other(ranks - step)),
        ):
            pl.when(there)(functools.partial(signal, barrier, device))
            greeted = greeted + there.astype(jnp.int32)
    for step in range(1, curve):
        signal(barrier, (lax.rem(my_curve + step, curve), my_group))

    def spread(index):
        for step in rounds_of(group)[index]:
            for there, to in (
                (my_group + step < group, my_group + step),
                (my_group >= step, my_group - step),
            ):
                pl.when(there)(functools.partial(signal, seen.at[index], (my_curve, to)))

    def gather(index):
        count = 0
        for step in rounds_of(group)[index]:
            count = count + (my_group + step < group).astype(jnp.int32)
            count = count + (my_group >= step).astype(jnp.int32)
        pl.semaphore_wait(seen.at[index], count)

    loads = [
        pltpu.make_async_copy(source, target, load_sem.at[index])
        for index, (source, target) in enumerate(
            (
                (dest_hbm, dest_ref),
                (list_hbm, list_ref),
                (cond_hbm, cond_ref),
                (rhs_hbm, rhs_ref),
                (forward_hbm, forward_ref),
                (neigh_hbm, neigh_ref),
                (orient_hbm, orient_ref),
                (column_hbm, column_ref),
                (backward_hbm, backward_ref),
            )
        )
    ]
    for load in loads:
        load.start()
    clear(1, (moved, tag_in, halo_in.at[0], halo_in.at[1]))
    clear(2, (far_in,))
    for load in loads[:4]:
        load.wait()

    def faces_of(stacked, kappa, first, last):
        part = dot(forward_ref[first * FACE : last * FACE, :], stacked)
        own, halves = [], []
        for index in range(last - first):
            value = part[index * FACE : index * FACE + PART]
            flux = kappa * part[index * FACE + PART : (index + 1) * FACE]
            own.append((value, flux))
            halves.append(jnp.concatenate(split_two(jnp.concatenate([value, flux], 0)), 0))
        return own, halves

    offset = dest_ref[...] - me * cells
    goes_left = offset < 0
    goes_right = offset >= cells
    slot = jnp.where(goes_left, offset + cells, jnp.where(goes_right, offset - cells, offset))
    payload[0:BLOCK, :] = rhs_ref[...]
    payload[KAPPA : KAPPA + 1, :] = cond_ref[...]
    payload[TAG : TAG + 1, :] = (slot + 1).astype(F32)
    payload[TAG + 1 : TAG + 2, :] = jnp.zeros((1, cells), F32)
    high, mid, low = split_three(payload[...])
    parts = jnp.concatenate([high, mid, low], 0)
    row8 = iota((8, cells), 0)
    leaving = jnp.where(
        row8 == 0,
        jnp.where(goes_left, 1.0, 0.0),
        jnp.where(row8 == 1, jnp.where(goes_right, 1.0, 0.0), 0.0),
    ).astype(BF)
    triangle = jnp.where(iota((cells, cells), 0) <= iota((cells, cells), 1), 1.0, 0.0).astype(BF)
    order = dot(leaving, triangle).astype(jnp.int32) - 1
    slots = iota((MOVE, cells), 0)
    pick = jnp.concatenate(
        [
            one_hot(jnp.where(goes_left, order[0:1], -1), slots),
            one_hot(jnp.where(goes_right, order[1:2], -1), slots),
        ],
        0,
    )
    chosen = dot_last(pick, parts)
    chosen = chosen[:, :ROWS] + chosen[:, ROWS : 2 * ROWS] + chosen[:, 2 * ROWS :]
    packed[0] = chosen[:MOVE]
    packed[1] = chosen[MOVE:]

    lists = list_ref[...].astype(F32)
    for side in range(2):
        tag_out[side] = lists[side : side + 1, :]

    pl.semaphore_wait(barrier, greeted)

    moves = Exchange(packed, moved, move_send, move_recv, 1)
    tags = Exchange(tag_out, tag_in, tag_send, tag_recv, 1)
    moves.start(0)
    pl.when(my_group > 0)(functools.partial(moves.start, 1))
    for side in range(2):
        tags.start(side)

    for load in loads[4:]:
        load.wait()

    old_halves = faces_of(jnp.concatenate([high, mid, high], 0), cond_ref[...], 0, 2)[1]
    offset_column = jnp.broadcast_to(offset.astype(F32), (8, cells)).T[:, 0:1]
    halo_rows = iota((HALO, ghost), 0)

    def shrink(out):
        out = out[:FACE] + out[FACE:]
        return jnp.where(halo_rows == FACE_LAST, out[HALO : HALO + 1], out[:HALO])

    def widen(message):
        last = message[FACE_LAST : FACE_LAST + 1]
        rest = jnp.where(iota((FACE - HALO, ghost), 0) == 0, last, 0.0)
        return jnp.concatenate([message, rest], 0)

    for side in range(2):
        hot = one_hot(offset_column, lists[side : side + 1, :])
        out = dot(old_halves[side], hot)
        halo_out[0, side] = shrink(out)
    lanes = iota((2 * MOVE, ROWS), 1)
    tagged = jnp.where(lanes == FACE_TAG, chosen[:, TAG : TAG + 1], 0.0)
    leaving_low = dot_last(pick, old_halves[0]) + tagged
    leaving_high = dot_last(pick, old_halves[1]) + tagged
    leaving_low = leaving_low[:, :FACE] + leaving_low[:, FACE:]
    leaving_high = leaving_high[:, :FACE] + leaving_high[:, FACE:]
    middle = MOVE // 2
    far_out[0] = jnp.concatenate([leaving_low[:middle], leaving_low[middle:MOVE]], 1)
    far_out[1] = jnp.concatenate([leaving_high[MOVE : MOVE + middle], leaving_high[MOVE + middle :]], 1)

    halos = Exchange(halo_out.at[0], halo_in.at[0], halo_send.at[0], halo_recv.at[0], 1)
    fars = Exchange(far_out, far_in, far_send, far_recv, 2)
    pl.when(my_group == 0)(functools.partial(halos.start, 0))
    pl.when(my_group > 0)(functools.partial(halos.start, 1))
    pl.when(my_group == 0)(functools.partial(moves.start, 1))
    for side in range(2):
        fars.start(side)

    stay = one_hot(iota((cells, cells), 0), offset)
    arrived = dot_last(parts, stay)
    cell_rows = iota((cells, cells), 0)
    ghost_rows = iota((ghost, cells), 0)
    for face in range(3):
        local_hot[face] = one_hot(neigh_ref[face : face + 1, :], cell_rows)
    pl.when(my_group == 0)(functools.partial(halos.start, 1))
    pl.when(my_group > 0)(functools.partial(halos.start, 0))
    spread(0)
    for face in range(3, 6):
        local_hot[face] = one_hot(neigh_ref[face : face + 1, :], cell_rows)
    for side in range(2):
        ghost_hot[side] = one_hot(
            neigh_ref[side : side + 1, :] - (cells + side * ghost), ghost_rows
        )
        send_hot[side] = one_hot(list_ref[side : side + 1, :], iota((cells, ghost), 0))

    def folded(value):
        half = value.shape[0] // 2
        return value[:half] + value[half:]

    arrived = arrived[:ROWS] + arrived[ROWS : 2 * ROWS] + arrived[2 * ROWS :]
    high, low = split_two(arrived)
    stay_halves = faces_of(
        jnp.concatenate([high, low, high], 0), arrived[KAPPA : KAPPA + 1], 0, 6
    )[1]
    for face in range(6):
        near_ref[face] = folded(dot(stay_halves[face ^ 1], local_hot[face]))
    payload[...] = arrived

    for side in range(2):
        moves.arrive(side)
        tags.arrive(side)
    record = moved[...].reshape(2 * MOVE, ROWS)
    landing = record[:, TAG : TAG + 1].astype(jnp.int32) - 1
    record = record.T
    high, mid, low = split_three(record)
    placed = dot(
        jnp.concatenate([high, mid, low], 0), one_hot(landing, iota((2 * MOVE, cells), 1))
    )
    arrived = payload[...] + (placed[:ROWS] + placed[ROWS : 2 * ROWS] + placed[2 * ROWS :])
    moved_halves = faces_of(
        jnp.concatenate([high, mid, high], 0), record[KAPPA : KAPPA + 1], 0, 6
    )[1]
    landing = jnp.where(landing < 0, -2, landing)

    def near_old(face):
        hot = one_hot(landing, neigh_ref[face : face + 1, :])
        return near_ref[face] + folded(dot(moved_halves[face ^ 1], hot))

    rows = iota((ROWS, cells), 0)
    field = jnp.where(rows < BLOCK, arrived, 0.0)
    kappa = arrived[KAPPA : KAPPA + 1]
    cell_weight = column_ref[:, 0:1]
    face_weight = column_ref[0:PART, 1:2]
    first_odd = column_ref[0:PART, 2:3]
    second_odd = column_ref[0:PART, 3:4]

    def signs(face):
        code = orient_ref[face : face + 1, :]
        first_bit = jnp.where(lax.rem(code, 2) == 1, 1.0, 0.0)
        second_bit = jnp.where(code >= 2, 1.0, 0.0)
        return (1.0 - first_odd * first_bit) * (1.0 - second_odd * second_bit)

    def outer(face):
        return jnp.where(neigh_ref[face : face + 1, :] < 0, 1.0, 0.0)

    def coefficients(face, own, near):
        value, flux = own
        sign = signs(face)
        outside = outer(face)
        near_kappa = near[FACE_KAPPA : FACE_KAPPA + 1] + outside * kappa
        penalty = PENALTY * jnp.maximum(kappa, near_kappa)
        jump = value - (sign * near[:PART] - outside * value)
        mean = flux - (sign * near[PART:] - outside * flux)
        scaled = -0.5 * (face_weight * jump)
        first = face_weight * (penalty * jump - 0.5 * mean)
        return (first, kappa * scaled), (jump, mean, first, scaled)

    def lifted(parts, first, last):
        high, low = parts
        both = dot(backward_ref[0 : 2 * ROWS, first * FACE : last * FACE], high)
        rest = dot(backward_ref[0:ROWS, first * FACE : last * FACE], low)
        return both[:ROWS] + both[ROWS:] + rest

    def traced(parts, first, last):
        high, low = parts
        both = dot(backward_ref[2 * ROWS :, first * FACE : last * FACE], high)
        rest = dot(backward_ref[2 * ROWS : 2 * ROWS + FACE, first * FACE : last * FACE], low)
        return both[:FACE] + both[FACE:] + rest

    def split_terms(terms):
        return split_two(jnp.concatenate(terms, 0))

    def stack(field):
        high, low = split_two(jnp.where(rows == KAPPA, kappa, field))
        return jnp.concatenate([high, low, high], 0)

    def inner(field, stacked, own, near):
        terms = []
        for face in range(2, 6):
            terms += coefficients(face, own[face], near(face))[0]
        stiff = dot(forward_ref[6 * FACE : 6 * FACE + ROWS, :], stacked)
        terms = split_terms(terms)
        result = lifted(terms, 2, 6) + cell_weight * field + kappa * stiff
        return result, [near(face) for face in range(2)], terms

    def with_ghosts(near, ghosts, side):
        return near + folded(dot(jnp.concatenate(split_two(ghosts), 0), ghost_hot[side]))

    def down(value):
        return jnp.sum(value, 0, keepdims=True)

    def across(value):
        return jnp.sum(value, 1, keepdims=True)

    basis[0] = field
    stacked = stack(field)
    own = faces_of(stacked, kappa, 0, 6)[0]
    result, near, terms = inner(field, stacked, own, near_old)
    volume = dot(forward_ref[6 * FACE + ROWS :, :], stacked)
    trace = traced(terms, 2, 6) + kappa * volume[:FACE] + volume[FACE:]
    marks = []
    for side in range(2):
        mark = jnp.concatenate(split_two(jnp.broadcast_to(tag_in[side] + 1.0, (8, ghost))), 0)
        mark = dot(mark, ghost_hot[side])
        mark = mark[0:1] + mark[8:9]
        marks.append(jnp.where(mark == 0.0, -1.0, mark))
    for side in range(2):
        halos.arrive(side)
        fars.arrive(side)
    gather(0)
    terms = []
    for face in range(2):
        gone = leaving_high[:MOVE] if face == 0 else leaving_low[MOVE:]
        far = far_in[face]
        wide = jnp.concatenate([far[:, :FACE], far[:, FACE:], gone], 0)
        hot = one_hot(wide[:, FACE_TAG : FACE_TAG + 1], marks[face])
        placed = dot(jnp.concatenate(split_two(wide.T), 0), hot)
        ghosts = with_ghosts(near[face], widen(halo_in[0, face]), face) + folded(placed)
        terms += coefficients(face, own[face], ghosts)[0]
    terms = split_terms(terms)
    trace = trace + traced(terms, 0, 2)
    value = jnp.where(iota((PART, cells), 0) == FACE_KAPPA, kappa, trace[:PART])
    parts = jnp.concatenate(split_two(jnp.concatenate([value, kappa * trace[PART:]], 0)), 0)
    halo_out[1, 1] = shrink(dot(parts, send_hot[1]))
    images = Exchange(halo_out.at[1], halo_in.at[1], halo_send.at[1], halo_recv.at[1], 1)
    report = pltpu.make_async_remote_copy(
        src_ref=halo_out.at[1, 1],
        dst_ref=edge_in,
        send_sem=edge_send.at[0],
        recv_sem=edge_recv.at[0],
        device_id=(my_curve, 0),
        device_id_type=MESH,
    )
    pl.when(reports)(report.start)
    images.start(1)
    if len(rounds_of(group)) > 1:
        spread(1)
    image = result + lifted(terms, 0, 2)
    basis[1] = image
    stacked = stack(image)
    own, halves = faces_of(stacked, kappa, 0, 6)
    result, near, _ = inner(
        image, stacked, own, lambda face: folded(dot(halves[face ^ 1], local_hot[face]))
    )
    halo_out[1, 0] = shrink(dot(halves[0], send_hot[0]))
    images.start(0)
    value, flux = own[1]
    edge = 2.0 * outer(1) * down(face_weight * (value * (PENALTY * kappa * value - flux)))
    found = [across(down(field * field)), across(down(field * image)), across(down(image * image))]
    outside = outer(0) > 0.0
    kept[...] = near[0]
    _, (jump, mean, first, scaled) = coefficients(0, own[0], near[0])

    inside = jnp.where(outside, own[0][0], jump) * first + jnp.where(outside, own[0][1], mean) * scaled
    inside = jnp.where(neigh_ref[0:1, :] < cells, down(inside), 0.0)
    found.append(across(down(image * result) + edge + inside))
    lane = iota((1, ROWS), 1)
    message = jnp.zeros((1, ROWS), F32)
    for index, value in enumerate(found):
        message = jnp.where(lax.rem(lane, 4) == index, value, message)
    across_edge = dot_last(halves[0], ghost_hot[0])
    across_edge = across_edge[:FACE] + across_edge[FACE:]
    code = orient_ref[0:1, :]
    bit_rows = iota((8, cells), 0)
    bits = jnp.where(
        bit_rows == 0, lax.rem(code, 2), jnp.where(bit_rows == 1, jnp.where(code >= 2, 1, 0), 1)
    )
    bits = dot_last(bits.astype(F32).astype(BF), ghost_hot[0])
    for index in range(3):
        row = iota((FACE, ghost), 0) == FACE_TAG + index
        across_edge = jnp.where(row, bits[index : index + 1], across_edge)
    slot_out[...] = across_edge
    defer = pltpu.make_async_remote_copy(
        src_ref=slot_out,
        dst_ref=slot_in,
        send_sem=edge_send.at[1],
        recv_sem=edge_recv.at[1],
        device_id=(lax.rem(my_curve + curve - 1, curve), my_group),
        device_id_type=MESH,
    )
    pl.when(defers)(defer.start)

    def edge_energy(mine, ghosts):
        bit = mine[FACE_TAG : FACE_TAG + 3]
        sign = (1.0 - first_odd * bit[0:1]) * (1.0 - second_odd * bit[1:2])
        kappas = jnp.maximum(mine[FACE_KAPPA : FACE_KAPPA + 1], ghosts[FACE_KAPPA : FACE_KAPPA + 1])
        jump = mine[:PART] - sign * ghosts[:PART]
        mean = mine[PART:] - sign * ghosts[PART:]
        energy = face_weight * bit[2:3] * (jump * (PENALTY * kappas * jump - mean))
        return jnp.broadcast_to(across(down(energy)), (1, ROWS))

    for index in range(1, len(rounds_of(group))):
        if index > 1:
            spread(index)
        if index < len(rounds_of(group)) - 1:
            gather(index)
    shared[...] = jnp.zeros((1, ROWS), F32)

    @pl.when(jnp.logical_not(defers))
    def _():
        images.arrive(0)
        shared[...] = edge_energy(slot_out[...], widen(halo_in[1, 0]))

    if len(rounds_of(group)) > 1:
        gather(len(rounds_of(group)) - 1)

    @pl.when(helps)
    def _():
        defer.wait_recv()
        report.wait_recv()
        shared[...] += edge_energy(slot_in[...], widen(edge_in[...]))

    sums[me] = message + jnp.where(lax.rem(lane, 4) == 3, shared[...], 0.0)

    for_each_other(
        lambda device: pltpu.make_async_remote_copy(
            src_ref=sums.at[me],
            dst_ref=sums.at[me],
            send_sem=sum_send,
            recv_sem=sum_recv,
            device_id=device,
            device_id_type=MESH,
        ).start()
    )

    pl.when(defers)(functools.partial(images.arrive, 0))
    images.arrive(1)
    pl.when(defers)(defer.wait_send)
    pl.when(reports)(report.wait_send)
    terms = []
    near[0] = kept[...]
    for face in range(2):
        terms += coefficients(face, own[face], with_ghosts(near[face], widen(halo_in[1, face]), face))[0]
    basis[2] = result + lifted(split_terms(terms), 0, 2)
    for copies in (moves, tags, halos, fars, images):
        copies.leave()
    rest = sums.at[pl.ds(1, ranks - 1)]
    pltpu.make_async_copy(rest, rest, sum_send).wait()
    pltpu.make_async_copy(rest, rest, sum_recv).wait()
    summed = jnp.sum(sums[...], 0)
    turns = [summed] + [pltpu.roll(summed, turn, 1) for turn in range(1, 4)]
    phase = lax.rem(lane, 4)
    totals = []
    for index in range(4):
        total = turns[3]
        for turn in range(3):
            total = jnp.where(lax.rem(phase + 4 - turn, 4) == index, turns[turn], total)
        totals.append(total)
    low, mid, high = (totals[index + 1] / totals[index] for index in range(3))
    scale = 1.0 / (low * mid * (high - mid))
    linear = mid * (high - low) * scale
    square = (mid - low) * scale
    linear_ref[...] = jnp.concatenate([linear] * (cells // ROWS), 1)
    square_ref[...] = jnp.concatenate([square] * (cells // ROWS), 1)


def body(shape, right_side, conductivity, destination, neighbour, orientation, send_list):
    cells = right_side.shape[1]
    ghost = send_list.shape[1]
    ranks = shape[0] * shape[1]
    forward, backward, columns = tables()
    vmem = pl.BlockSpec(memory_space=pltpu.VMEM)
    dma = pltpu.SemaphoreType.DMA
    operands = (
        right_side,
        conductivity[None],
        destination[None],
        neighbour,
        orientation,
        send_list,
        jnp.asarray(forward),
        jnp.asarray(backward),
        jnp.asarray(columns),
    )
    operands = tuple(pltpu.with_memory_space_constraint(item, pltpu.HBM) for item in operands)
    basis, linear, square = pl.pallas_call(
        functools.partial(kernel, shape),
        out_shape=(
            jax.ShapeDtypeStruct((3, ROWS, cells), F32),
            jax.ShapeDtypeStruct((1, cells), F32),
            jax.ShapeDtypeStruct((1, cells), F32),
        ),
        in_specs=[pl.BlockSpec(memory_space=pltpu.HBM)] * len(operands),
        out_specs=(vmem, vmem, vmem),
        scratch_shapes=[pltpu.VMEM(item.shape, item.dtype) for item in operands]
        + [
            pltpu.VMEM((ROWS, cells), F32),
            pltpu.VMEM((6, cells, cells), BF),
            pltpu.VMEM((2, ghost, cells), BF),
            pltpu.VMEM((2, cells, ghost), BF),
            pltpu.VMEM((2, MOVE, ROWS), F32),
            pltpu.VMEM((2, MOVE, ROWS), F32),
            pltpu.VMEM((2, MOVE // 2, ROWS), F32),
            pltpu.VMEM((2, MOVE // 2, ROWS), F32),
            pltpu.VMEM((2, 2, HALO, ghost), F32),
            pltpu.VMEM((2, 2, HALO, ghost), F32),
            pltpu.VMEM((ranks, 1, ROWS), F32),
            pltpu.VMEM((FACE, cells), F32),
            pltpu.VMEM((1, ROWS), F32),
            pltpu.VMEM((FACE, ghost), F32),
            pltpu.VMEM((FACE, ghost), F32),
            pltpu.VMEM((HALO, ghost), F32),
            dma((2,)),
            dma((2,)),
            pltpu.VMEM((6, FACE, cells), F32),
            pltpu.VMEM((2, 1, ghost), F32),
            pltpu.VMEM((2, 1, ghost), F32),
            dma((2,)),
            dma((2,)),
            dma((len(operands),)),
            dma((2,)),
            dma((2,)),
            dma((2,)),
            dma((2,)),
            dma((2, 2)),
            dma((2, 2)),
            dma,
            dma,
            pltpu.SemaphoreType.REGULAR((len(rounds_of(shape[1])),)),
        ],
        compiler_params=pltpu.CompilerParams(
            collective_id=0, has_side_effects=True, vmem_limit_bytes=VMEM_LIMIT
        ),
    )(*operands)
    first, second, third = (basis[index, :BLOCK] for index in range(3))
    return linear * first - square * second, first - linear * second + square * third


def solution(mesh):
    both = ("curve", "group")
    shape = (mesh.shape["curve"], mesh.shape["group"])
    in_specs = (P(None, both), P(both), P(both), P(None, both), P(None, both), P(None, both))
    out_specs = (P(None, both), P(None, both))
    return jax.shard_map(
        functools.partial(body, shape),
        mesh=mesh,
        in_specs=in_specs,
        out_specs=out_specs,
        check_vma=False,
    )
```
